32 devices in a mesh: dp: 8 (over z, x), seq: 4 (over y, core).
Axes of the slice: x: 2, y: 2, z: 4, core: 2. Of those that a mesh axis runs over, the one named last changes fastest.
Arguments:
- queries: bfloat16 [4096, 2048], P(('dp', 'seq')), may hold values from -6 to 6
- keys: bfloat16 [4096, 2048], P(('dp', 'seq')), may hold values from -6 to 6
- values: bfloat16 [4096, 2048], P(('dp', 'seq')), may hold values from -6 to 6
- q_gain: float32 [2048], replicated, may hold values from 0.25 to 1.75
- k_gain: float32 [2048], replicated, may hold values from 0.25 to 1.75
- out_grad: bfloat16 [4096, 2048], P(('dp', 'seq')), may hold values from -16 to 16
- segments: int32 [8, 512], P('dp'), may hold values from 0 to 3, never falling along the last dimension, each value on 1 to 256 neighbouring positions
- visible: int32 [8, 512], P('dp'), may hold values 0 or 1
Outputs:
- attn_out: bfloat16 [4096, 2048], P(('dp', 'seq'))
- query_grad: bfloat16 [4096, 2048], P(('dp', 'seq'))
- key_grad: bfloat16 [4096, 2048], P(('dp', 'seq'))
- value_grad: bfloat16 [4096, 2048], P(('dp', 'seq'))
- q_gain_grad: float32 [2048], replicated
- k_gain_grad: float32 [2048], replicated
The draws below stay inside these ranges and needn't reach their ends.
Inputs may be any that keep to these rules, and one draw needn't show every extreme that they name: `segments`: along each packed sequence the clip numbers never fall; each of the 4 clips holds 1 to 256 slots.
All inputs are finite; a program needn't handle non-finite values. No bound on the sum of `visible` on one device may be relied on, other than what follows from the above.
Results may differ from the reference program's by a relative error of at most 0.012.
The reference program's roundings to bfloat16 on the way (of `prob_half` and `score_grad`) count: a program that leaves them out, or rounds other values in their place, can miss the bound.
Values may be sent and summed in bfloat16 or wider, within the bound.
No kernel may reach another device: no remote copies, remote signals or barrier semaphores. Data moves between devices by JAX's collectives and lax.ppermute only.
A program may use at most 64 MiB of HBM per device.

```python
import math
import jax
import jax.numpy as jnp
import numpy as np
from jax import lax

HEADS = 16
D_HEAD = 128
CLIPS = 4
WIDTH = 2048
SEQ_LEN = 512
TOKENS = 4096
N_DP = 8


def draw_queries(key, part):
    drawn = jax.random.normal(jax.random.fold_in(key, 11), (TOKENS, HEADS * D_HEAD), jnp.float32)
    return jnp.clip(drawn, -6.0, 6.0).astype(jnp.bfloat16)


def draw_keys(key, part):
    drawn = jax.random.normal(jax.random.fold_in(key, 23), (TOKENS, HEADS * D_HEAD), jnp.float32)
    return jnp.clip(drawn, -6.0, 6.0).astype(jnp.bfloat16)


def place_ends(values, stream_key, least, top_value):
    longest = values.shape.index(max(values.shape))
    spots = []
    for shift in (0, 1):
        where = [jax.random.randint(jax.random.fold_in(stream_key, axis), (), 0, length) for axis, length in enumerate(values.shape)]
        where[longest] = (where[longest] + shift) % values.shape[longest]
        spots.append(tuple(where))
    return values.at[spots[0]].set(least).at[spots[1]].set(top_value)


def block_scale(own_key, extent, split, smallest, largest):
    level, own = 1.0, jax.random.fold_in(own_key, 6)
    for axis_at, parts in split:
        steps = jnp.exp(jax.random.uniform(jax.random.fold_in(own, axis_at), (parts,), jnp.float32, smallest / len(split), largest / len(split)))
        level = level * jnp.repeat(steps, extent[axis_at] // parts).reshape([-1 if axis == axis_at else 1 for axis in range(len(extent))])
    return level


def profile(amount, total, most, skew):
    loads = [(1 << 20) // math.isqrt(grade ** skew) + 1 for grade in range(2, amount + 1)]
    spare, holding = total - most - (amount - 1), [1] * (amount - 1)
    while spare > 0:
        movable = [i for i in range(amount - 1) if holding[i] < most]
        mass, left = sum([loads[i] for i in movable]), spare
        for i in movable:
            addition = min(most - holding[i], max(1, left * loads[i] // mass), spare)
            holding[i] = holding[i] + addition
            spare = spare - addition
    return np.array([most] + holding)


def uneven(own_key, count, total, most, slope):
    if count == 2:
        one = jax.random.randint(own_key, (), max(1, total - most), min(most, total - 1) + 1)
        return jnp.stack([one, total - one])
    lengths = jnp.asarray(profile(count, total, most, slope), jnp.int32)
    pairs = (count - 1) // 2
    source_of, receiver = lengths[1:1 + 2 * pairs:2], lengths[2:2 + 2 * pairs:2]
    room = jnp.minimum(source_of - 1, most - receiver)
    shifted = jax.random.randint(jax.random.fold_in(own_key, 1), (pairs,), 0, 1 << 20) % (room + 1)
    lengths = lengths.at[1:1 + 2 * pairs:2].set(source_of - shifted).at[2:2 + 2 * pairs:2].set(receiver + shifted)
    return lengths[jax.random.permutation(jax.random.fold_in(own_key, 2), count)]


def normal_values(key, extent, scale, reach, pieces=(), kind=jnp.bfloat16):
    loudness = block_scale(key, extent, pieces, -0.22, 0.18) if pieces else 1.0
    values = jax.random.normal(key, extent, jnp.float32) * scale * loudness
    return jnp.minimum(jnp.maximum(values, -reach), reach).astype(kind)


def setup_inputs(seed: int = 0) -> dict:
    splits = jax.random.split(jax.random.key(seed), 9)
    queries = draw_queries(jax.random.fold_in(splits[8], 71), 0)
    keys = draw_keys(jax.random.fold_in(splits[8], 71), 0)
    values = normal_values(splits[2], (TOKENS, WIDTH), 1.0, 6.0, ((0, 32),))
    q_gain = jnp.clip(1.0 + 0.15 * jax.random.normal(splits[3], (WIDTH,), jnp.float32), 0.25, 1.75)
    k_gain = jnp.clip(1.0 + 0.15 * jax.random.normal(splits[4], (WIDTH,), jnp.float32), 0.25, 1.75)
    out_grad = normal_values(splits[5], (TOKENS, WIDTH), 4.0, 16.0, ((0, 32),))
    segments = jax.vmap(lambda own: jnp.searchsorted(jnp.cumsum(uneven(own, CLIPS, SEQ_LEN, SEQ_LEN // 2, 2)), jnp.arange(SEQ_LEN), side="right"))(jax.random.split(splits[6], N_DP)).reshape((N_DP, SEQ_LEN)).astype(jnp.int32)
    visible = place_ends((jax.random.randint(splits[7], (N_DP, SEQ_LEN), 0, 5) < 4).astype(jnp.int32), jax.random.fold_in(splits[7], 1), 0, 1)
    return dict(queries=queries, keys=keys, values=values, q_gain=q_gain, k_gain=k_gain, out_grad=out_grad, segments=segments, visible=visible)


epsilon = 1e-06

def normalize(raw_rows, gain_vec):
    raw_f32 = raw_rows.astype(jnp.float32)
    inv_rms = lax.rsqrt(lax.optimization_barrier(jnp.mean(raw_f32 * raw_f32, axis=-1, keepdims=True)) + epsilon)
    return ((raw_f32 * inv_rms * gain_vec).astype(jnp.bfloat16), inv_rms)

def norm_back(raw_rows, inv_rms, gain_vec, grad_norm):
    raw_f32 = raw_rows.astype(jnp.float32)
    grad_f32 = grad_norm.astype(jnp.float32)
    scaled_grad = gain_vec * grad_f32
    mean_term = lax.optimization_barrier(jnp.mean(scaled_grad * raw_f32, axis=-1, keepdims=True))
    grad_raw = inv_rms * scaled_grad - raw_f32 * inv_rms ** 3 * mean_term
    return (grad_raw.astype(jnp.bfloat16), lax.optimization_barrier(jnp.sum(grad_f32 * raw_f32 * inv_rms, axis=0)))

def attend(items):
    q_norm, k_norm, val_rows, grad_rows, seg_row, vis_row = items
    seq_rows = q_norm.shape[0]
    score_scale = D_HEAD ** (-0.5)
    q_three = q_norm.reshape(seq_rows, HEADS, D_HEAD).astype(jnp.float32)
    k_three = k_norm.reshape(seq_rows, HEADS, D_HEAD).astype(jnp.float32)
    v_three = val_rows.reshape(seq_rows, HEADS, D_HEAD).astype(jnp.float32)
    grad_three = grad_rows.reshape(seq_rows, HEADS, D_HEAD).astype(jnp.float32)
    positions = jnp.arange(seq_rows, dtype=jnp.int32)
    allowed = (seg_row[:, None] == seg_row[None, :]) & ((vis_row[None, :] == 1) | (positions[:, None] == positions[None, :]))
    scores = jnp.einsum('shd,thd->hst', q_three, k_three) * score_scale
    scores = jnp.where(allowed[None], scores, -1e+30)
    row_max = lax.optimization_barrier(jnp.max(scores, axis=-1, keepdims=True))
    weights = jnp.exp(scores - row_max)
    attn_prob = weights / lax.optimization_barrier(jnp.sum(weights, axis=-1, keepdims=True))
    prob_half = lax.optimization_barrier(attn_prob.astype(jnp.bfloat16)).astype(jnp.float32)
    attn_out = jnp.einsum('hst,thd->shd', prob_half, v_three).reshape(seq_rows, WIDTH).astype(jnp.bfloat16)
    dprob = jnp.einsum('shd,thd->hst', grad_three, v_three)
    val_grad = jnp.einsum('hst,shd->thd', prob_half, grad_three).reshape(seq_rows, WIDTH).astype(jnp.bfloat16)
    row_dot = lax.optimization_barrier(jnp.sum(attn_prob * dprob, axis=-1, keepdims=True))
    score_grad = attn_prob * (dprob - row_dot) * score_scale
    score_grad = lax.optimization_barrier(score_grad.astype(jnp.bfloat16)).astype(jnp.float32)
    q_grad = jnp.einsum('hst,thd->shd', score_grad, k_three).reshape(seq_rows, WIDTH).astype(jnp.bfloat16)
    k_grad = jnp.einsum('hst,shd->thd', score_grad, q_three).reshape(seq_rows, WIDTH).astype(jnp.bfloat16)
    return (attn_out, q_grad, k_grad, val_grad)

def reference(queries, keys, values, q_gain, k_gain, out_grad, segments, visible):
    q_norm, q_inv = normalize(queries, q_gain)
    k_norm, k_inv = normalize(keys, k_gain)

    def packed(array):
        return array.reshape(N_DP, SEQ_LEN, WIDTH)
    results = lax.map(attend, (packed(q_norm), packed(k_norm), packed(values), packed(out_grad), segments, visible))
    attn_out, q_grad, k_grad, val_grad = [packed_out.reshape(TOKENS, WIDTH) for packed_out in results]
    query_grad, q_gain_grad = norm_back(queries, q_inv, q_gain, q_grad)
    key_grad, k_gain_grad = norm_back(keys, k_inv, k_gain, k_grad)
    return (attn_out, query_grad, key_grad, val_grad, q_gain_grad, k_gain_grad)
```

```python
import functools

import jax
import jax.numpy as jnp
from jax import lax
from jax.experimental import pallas as pl
from jax.experimental.pallas import tpu as pltpu
from jax.sharding import PartitionSpec as P

D_HEAD = 128
UNIT = 16
CORES = 2
EPSILON = 1e-06
NEG = -1e30


def normalize(raw_rows, gain_vec):
    raw_f32 = raw_rows.astype(jnp.float32)
    inv_rms = lax.rsqrt(jnp.mean(raw_f32 * raw_f32, axis=-1, keepdims=True) + EPSILON)
    return ((raw_f32 * inv_rms * gain_vec).astype(jnp.bfloat16), inv_rms)


def norm_back(raw_rows, inv_rms, gain_vec, grad_norm):
    raw_f32 = raw_rows.astype(jnp.float32)
    grad_f32 = grad_norm.astype(jnp.float32)
    scaled_grad = gain_vec * grad_f32
    mean_term = jnp.mean(scaled_grad * raw_f32, axis=-1, keepdims=True)
    grad_raw = inv_rms * scaled_grad - raw_f32 * inv_rms**3 * mean_term
    return (grad_raw.astype(jnp.bfloat16), jnp.sum(grad_f32 * raw_f32 * inv_rms, axis=0))


def attend(q_norm, k_norm, val_rows, grad_rows, seg_row, vis_row):
    seq_rows, feature_count = q_norm.shape
    heads = feature_count // D_HEAD
    scale = D_HEAD ** (-0.5)
    positions = jnp.arange(seq_rows, dtype=jnp.int32)
    allowed = (seg_row[:, None] == seg_row[None, :]) & (
        (vis_row[None, :] == 1) | (positions[:, None] == positions[None, :])
    )
    f32 = jnp.float32
    q, k, v, g = (
        x.reshape(seq_rows, heads, D_HEAD) for x in (q_norm, k_norm, val_rows, grad_rows)
    )
    scores = jnp.einsum("shd,thd->hst", q, k, preferred_element_type=f32) * scale
    scores = jnp.where(allowed[None], scores, NEG)
    weights = jnp.exp(scores - jnp.max(scores, axis=-1, keepdims=True))
    prob = weights / jnp.sum(weights, axis=-1, keepdims=True)
    half = prob.astype(jnp.bfloat16)
    out = jnp.einsum("hst,thd->shd", half, v, preferred_element_type=f32)
    dprob = jnp.einsum("shd,thd->hst", g, v, preferred_element_type=f32)
    v_grad = jnp.einsum("hst,shd->thd", half, g, preferred_element_type=f32)
    row_dot = jnp.sum(prob * dprob, axis=-1, keepdims=True)
    score_grad = (prob * (dprob - row_dot) * scale).astype(jnp.bfloat16)
    q_grad = jnp.einsum("hst,thd->shd", score_grad, k, preferred_element_type=f32)
    k_grad = jnp.einsum("hst,shd->thd", score_grad, q, preferred_element_type=f32)
    return tuple(
        x.reshape(seq_rows, feature_count).astype(jnp.bfloat16)
        for x in (out, q_grad, k_grad, v_grad)
    )


def per_device_any(queries, keys, values, q_gain, k_gain, out_grad, segments, visible):
    q_norm, q_inv = normalize(queries, q_gain)
    k_norm, k_inv = normalize(keys, k_gain)
    gather = functools.partial(
        lax.all_to_all, axis_name="seq", split_axis=1, concat_axis=0, tiled=True
    )
    spread = functools.partial(
        lax.all_to_all, axis_name="seq", split_axis=0, concat_axis=1, tiled=True
    )
    parts = attend(
        *(gather(x) for x in (q_norm, k_norm, values, out_grad)), segments[0], visible[0]
    )
    attn_out, q_grad, k_grad, value_grad = (spread(x) for x in parts)
    query_grad, q_gain_part = norm_back(queries, q_inv, q_gain, q_grad)
    key_grad, k_gain_part = norm_back(keys, k_inv, k_gain, k_grad)
    q_gain_grad, k_gain_grad = lax.psum((q_gain_part, k_gain_part), ("dp", "seq"))
    return (attn_out, query_grad, key_grad, value_grad, q_gain_grad, k_gain_grad)


def units_needed(blocks, heads):
    worst = 0
    for ka in range(1, blocks + 1):
        for kb in range(1, blocks + 2 - ka):
            worst = max(worst, min(max(ka * (heads - h), kb * h) for h in range(heads + 1)))
    return worst


def dot(x, y, dims):
    return lax.dot_general(x, y, (dims, ((), ())), preferred_element_type=jnp.float32)


NT = ((1,), (1,))
NN = ((1,), (0,))
TN = ((0,), (0,))


def attention(q, k, v, g, bias):
    scale = D_HEAD ** (-0.5)
    scores = dot(q, k, NT) * scale + bias
    weights = jnp.exp(scores - jnp.max(scores, axis=-1, keepdims=True))
    prob = weights * (1.0 / jnp.sum(weights, axis=-1, keepdims=True))
    half = prob.astype(jnp.bfloat16)
    out = dot(half, v, NN)
    dprob = dot(g, v, NT)
    v_grad = dot(half, g, TN)
    row_dot = jnp.sum(prob * dprob, axis=-1, keepdims=True)
    score_grad = (prob * (dprob - row_dot) * scale).astype(jnp.bfloat16)
    q_grad = dot(score_grad, k, NN)
    k_grad = dot(score_grad, q, TN)
    return tuple(x.astype(jnp.bfloat16) for x in (out, q_grad, k_grad, v_grad))


def own_side(plan):
    first = plan[0] == 0
    heads = plan[8]
    j0 = jnp.where(first, plan[6], 0)
    j1 = jnp.where(first, heads, plan[6])
    k_own = jnp.where(first, plan[4], plan[5])
    row0 = jnp.where(first, plan[9] - UNIT * plan[4], 0)
    return j0, j1, k_own, row0


def prepare_kernel(rows, heads, budget, q_ref, k_ref, v_ref, g_ref, qg_ref, kg_ref, seg_ref,
                   mine_ref, theirs_ref, inv_ref, plan_ref):
    core = lax.rem(lax.axis_index("seq"), CORES)
    half = heads * D_HEAD

    def put(i, normed):
        left = [normed[:, j * D_HEAD : (j + 1) * D_HEAD] for j in range(2 * heads)]

        @pl.when(core == 0)
        def _():
            for j in range(heads):
                mine_ref[i, j] = left[j]
                theirs_ref[i, j] = left[heads + j]

        @pl.when(core == 1)
        def _():
            for j in range(heads):
                mine_ref[i, j] = left[heads + j]
                theirs_ref[i, j] = left[j]

    for i, (raw_ref, gain_ref) in enumerate(((q_ref, qg_ref), (k_ref, kg_ref))):
        raw = raw_ref[...].astype(jnp.float32)
        inv = lax.rsqrt(jnp.mean(raw * raw, axis=-1, keepdims=True) + EPSILON)
        inv_ref[i] = jnp.broadcast_to(inv, inv_ref.shape[1:])
        put(i, (raw * inv * gain_ref[...]).astype(jnp.bfloat16))
    put(2, v_ref[...])
    put(3, g_ref[...])

    @pl.when(pl.program_id(0) == 0)
    def _():
        seg = seg_ref[...].astype(jnp.float32)
        chip_rows = seg.shape[1] // 2
        at = lax.broadcasted_iota(jnp.int32, seg.shape, 1)
        edge = jnp.sum(jnp.where(at == chip_rows - 1, seg, 0.0))
        beyond = jnp.sum(jnp.where(at == chip_rows, seg, 0.0))
        crosses = edge == beyond
        same = seg == edge
        a = jnp.sum(jnp.where(same & (at < chip_rows), 1.0, 0.0)).astype(jnp.int32)
        b = jnp.sum(jnp.where(same & (at >= chip_rows), 1.0, 0.0)).astype(jnp.int32)
        a = jnp.where(crosses, a, 0)
        b = jnp.where(crosses, b, 0)
        ka = lax.div(a + UNIT - 1, UNIT)
        kb = lax.div(b + UNIT - 1, UNIT)
        least = jnp.int32(0)
        most = jnp.int32(0)
        for h in range(heads):
            least += (ka * (heads - h) > budget).astype(jnp.int32)
            most += (kb * (h + 1) <= budget).astype(jnp.int32)
        plan_ref[0] = lax.div(lax.axis_index("seq"), CORES)
        plan_ref[1] = core
        plan_ref[2] = a
        plan_ref[3] = b
        plan_ref[4] = ka
        plan_ref[5] = kb
        plan_ref[6] = jnp.minimum(jnp.maximum(heads // 2, least), most)
        plan_ref[7] = crosses.astype(jnp.int32)
        plan_ref[8] = jnp.int32(heads)
        plan_ref[9] = jnp.int32(chip_rows)


def pack_kernel(rows, heads, plan, mine_ref, got_ref, send_ref):
    send_ref[...] = jnp.zeros_like(send_ref)
    core = plan[1]
    j0, j1, k_own, row0 = own_side(plan)
    for ref, half in ((mine_ref, core), (got_ref, 1 - core)):
        base = half * rows
        low = jnp.clip(lax.div(base - row0, UNIT), 0, k_own)
        high = jnp.clip(lax.div(base + rows - row0, UNIT), 0, k_own)

        def one_head(j, _, ref=ref, base=base, low=low, high=high):
            def one_unit(i, _):
                at = pl.multiple_of(row0 + UNIT * i - base, UNIT)
                to = pl.multiple_of(((j - j0) * k_own + i) * UNIT, UNIT)
                for n in range(4):
                    send_ref[n, pl.ds(to, UNIT), :] = ref[n, j, pl.ds(at, UNIT), :]
                return 0

            return lax.fori_loop(low, high, one_unit, 0)

        lax.fori_loop(j0, j1, one_head, 0)


def local_kernel(rows, plan, mine_ref, got_ref, seg_ref, vis_ref, keep_ref, give_ref, gain_ref,
                 bias_ref, ok_ref):
    both = 2 * rows

    @pl.when(pl.program_id(0) == 0)
    def _():
        core, first = plan[1], plan[0] * both

        def chip_row(ref):
            wide = ref[...].astype(jnp.float32)
            total = wide.shape[1]
            wide = jnp.broadcast_to(wide, (8, total))
            own = pltpu.roll(wide, lax.rem(2 * total - first - core * rows, total), 1)[:, :rows]
            other = pltpu.roll(wide, lax.rem(2 * total - first - (1 - core) * rows, total), 1)[:, :rows]
            return jnp.concatenate([own, other], axis=1)[0:1]

        seg = jnp.broadcast_to(chip_row(seg_ref), (both, both))
        vis = chip_row(vis_ref) > 0.5
        seg_t = jnp.transpose(seg)
        i = lax.broadcasted_iota(jnp.int32, (both, both), 0)
        j = lax.broadcasted_iota(jnp.int32, (both, both), 1)
        allowed = (seg == seg_t) & (vis | (i == j))
        bias_ref[...] = jnp.where(allowed, 0.0, NEG)
        r = lax.broadcasted_iota(jnp.int32, (both, D_HEAD), 0)
        at = jnp.where(r < rows, core * rows + r, (1 - core) * rows + r - rows) + first
        edge = plan[9]
        crossing = (at >= edge - plan[2]) & (at < edge + plan[3])
        ok_ref[...] = jnp.where(crossing, 0.0, 1.0)

    q, k, v, g = (
        jnp.concatenate([mine_ref[n, 0], got_ref[n, 0]], axis=0) for n in range(4)
    )
    out, q_grad, k_grad, v_grad = attention(q, k, v, g, bias_ref[...])
    for n, x in enumerate((out, q_grad, k_grad, v_grad)):
        keep_ref[n, 0] = x[:rows]
        give_ref[n, 0] = x[rows:]
    ok = ok_ref[...] > 0.5
    for n, (x, y) in enumerate(((q, q_grad), (k, k_grad))):
        term = jnp.where(ok, x.astype(jnp.float32) * y.astype(jnp.float32), 0.0)
        gain_ref[0, n : n + 1, :] = jnp.sum(term, axis=0, keepdims=True)


def crossing_kernel(rows, plan, mine_ref, got_ref, far_ref, vis_ref, keep_in, give_in, gain_in,
                    keep_ref, give_ref, gain_ref, back_ref, seq_ref, res_ref, bias_ref, n_ref):
    both = 2 * rows
    j = pl.program_id(0)
    chip, core = plan[0], plan[1]
    a, b = plan[2], plan[3]
    first = chip == 0
    edge = plan[9]
    start = edge - a
    own_lo = chip * both
    k_far = jnp.where(first, plan[5], plan[4])
    far_row0 = jnp.where(first, edge, edge - UNIT * plan[4])

    @pl.when(j == 0)
    def _():
        back_ref[...] = jnp.zeros_like(back_ref)
        seq_ref[...] = jnp.zeros_like(seq_ref)
        wide = vis_ref[...].astype(jnp.float32)
        total = wide.shape[1]
        vis = pltpu.roll(jnp.broadcast_to(wide, (8, total)), lax.rem(total - start, total), 1)
        vis = vis[0:1, :both] > 0.5
        r = lax.broadcasted_iota(jnp.int32, (both, both), 0)
        c = lax.broadcasted_iota(jnp.int32, (both, both), 1)
        allowed = (r == c) | ((r < a + b) & (c < a + b) & vis)
        bias_ref[...] = jnp.where(allowed, 0.0, NEG)

    ours = (plan[7] == 1) & jnp.where(first, j < plan[6], j >= plan[6])
    jj = jnp.where(first, j, j - plan[6])

    @pl.when(jnp.logical_not(ours))
    def _():
        keep_ref[...] = keep_in[...]
        give_ref[...] = give_in[...]
        gain_ref[...] = gain_in[...]

    @pl.when(ours)
    def _():
        own_at = pl.multiple_of(own_lo + core * rows, rows)
        got_at = pl.multiple_of(own_lo + (1 - core) * rows, rows)
        for n in range(4):
            seq_ref[n, pl.ds(own_at, rows), :] = mine_ref[n, 0].astype(jnp.float32)
            seq_ref[n, pl.ds(got_at, rows), :] = got_ref[n, 0].astype(jnp.float32)

        def load(i, _):
            at = pl.multiple_of((jj * k_far + i) * UNIT, UNIT)
            to = pl.multiple_of(far_row0 + UNIT * i, UNIT)
            for n in range(4):
                seq_ref[n, pl.ds(to, UNIT), :] = far_ref[n, pl.ds(at, UNIT), :].astype(jnp.float32)
            return 0

        lax.fori_loop(0, k_far, load, 0)
        q, k, v, g = (seq_ref[n, pl.ds(start, both), :].astype(jnp.bfloat16) for n in range(4))
        results = attention(q, k, v, g, bias_ref[...])
        for n, x in enumerate(results):
            res_ref[n, pl.ds(start, both), :] = x.astype(jnp.float32)
        r = lax.broadcasted_iota(jnp.int32, (both, D_HEAD), 0)
        for n, (x, y) in enumerate(((q, results[1]), (k, results[2]))):
            term = jnp.where(r < a + b, x.astype(jnp.float32) * y.astype(jnp.float32), 0.0)
            gain_ref[0, n : n + 1, :] = gain_in[0, n : n + 1, :] + jnp.sum(term, axis=0, keepdims=True)
        r = lax.broadcasted_iota(jnp.int32, (rows, D_HEAD), 0)
        for at, old, new in ((own_at, keep_in, keep_ref), (got_at, give_in, give_ref)):
            inside = (r + at >= start) & (r + at < edge + b)
            for n in range(4):
                x = res_ref[n, pl.ds(at, rows), :]
                new[n, 0] = jnp.where(inside, x, old[n, 0].astype(jnp.float32)).astype(jnp.bfloat16)

        def store(i, _):
            to = pl.multiple_of((jj * k_far + i) * UNIT, UNIT)
            at = pl.multiple_of(far_row0 + UNIT * i, UNIT)
            for n in range(4):
                back_ref[n, pl.ds(to, UNIT), :] = res_ref[n, pl.ds(at, UNIT), :].astype(jnp.bfloat16)
            return 0

        lax.fori_loop(0, k_far, store, 0)


def finish_kernel(rows, heads, plan, q_ref, k_ref, qg_ref, kg_ref, inv_ref, keep_ref, got_ref,
                  back_ref, back_got_ref, out_ref, dq_ref, dk_ref, dv_ref, gq_ref, gk_ref):
    core = plan[1]
    j0, j1, k_own, row0 = own_side(plan)
    base = core * rows
    low = jnp.clip(lax.div(base - row0, UNIT), 0, k_own)
    high = jnp.clip(lax.div(base + rows - row0, UNIT), 0, k_own)
    inside_lo = jnp.where(plan[0] == 0, plan[9] - plan[2], 0) - base
    inside_hi = jnp.where(plan[0] == 0, plan[9], plan[3]) - base
    targets = (out_ref, gq_ref, gk_ref, dv_ref)
    for ref, back, side in ((keep_ref, back_ref, core), (got_ref, back_got_ref, 1 - core)):
        for j in range(heads):
            col = pl.multiple_of((side * heads + j) * D_HEAD, D_HEAD)
            for n in range(4):
                targets[n][:, pl.ds(col, D_HEAD)] = ref[n, j]

        def one_head(j, _, back=back, side=side):
            col = pl.multiple_of((side * heads + j) * D_HEAD, D_HEAD)

            def one_unit(i, _):
                to = pl.multiple_of(row0 + UNIT * i - base, UNIT)
                at = pl.multiple_of(((j - j0) * k_own + i) * UNIT, UNIT)
                r = lax.broadcasted_iota(jnp.int32, (UNIT, D_HEAD), 0) + to
                inside = (r >= inside_lo) & (r < inside_hi)
                for n in range(4):
                    new = back[n, pl.ds(at, UNIT), :].astype(jnp.float32)
                    old = targets[n][pl.ds(to, UNIT), pl.ds(col, D_HEAD)].astype(jnp.float32)
                    targets[n][pl.ds(to, UNIT), pl.ds(col, D_HEAD)] = jnp.where(
                        inside, new, old
                    ).astype(jnp.bfloat16)
                return 0

            return lax.fori_loop(low, high, one_unit, 0)

        lax.fori_loop(j0, j1, one_head, 0)
    for n, (raw_ref, gain_ref, grad_ref, to_ref) in enumerate(
        ((q_ref, qg_ref, gq_ref, dq_ref), (k_ref, kg_ref, gk_ref, dk_ref))
    ):
        raw = raw_ref[...].astype(jnp.float32)
        scaled = gain_ref[...] * grad_ref[...].astype(jnp.float32)
        mean_term = jnp.mean(scaled * raw, axis=-1, keepdims=True)
        inv = inv_ref[n, :, 0:1]
        to_ref[...] = (inv * scaled - raw * (inv * inv * inv * mean_term)).astype(jnp.bfloat16)


def per_device_clips(queries, keys, values, q_gain, k_gain, out_grad, segments, visible, dp):
    rows, width = queries.shape
    heads = width // D_HEAD // CORES
    seq = segments.shape[1]
    blocks = CORES * rows // UNIT
    budget = units_needed(blocks, heads)
    both = CORES * rows
    bf16, f32 = jnp.bfloat16, jnp.float32
    shape = jax.ShapeDtypeStruct
    smem = pl.BlockSpec(memory_space=pltpu.SMEM)
    vmem = pl.BlockSpec(memory_space=pltpu.VMEM)
    swap_core = [(i, i ^ 1) for i in range(4)]
    swap_chip = [(i, i ^ 2) for i in range(4)]
    q_gain2, k_gain2 = q_gain[None], k_gain[None]

    steps = 2
    part = rows // steps
    row_spec = pl.BlockSpec((part, width), lambda i: (i, 0))
    gain_spec = pl.BlockSpec((1, width), lambda i: (0, 0))
    head_spec = pl.BlockSpec((4, heads, part, D_HEAD), lambda i: (0, 0, i, 0))
    mine, theirs, inv, plan = pl.pallas_call(
        functools.partial(prepare_kernel, rows, heads, budget),
        grid=(steps,),
        in_specs=[row_spec] * 4 + [gain_spec] * 2 + [pl.BlockSpec((1, seq), lambda i: (0, 0))],
        out_specs=[
            head_spec,
            head_spec,
            pl.BlockSpec((2, part, D_HEAD), lambda i: (0, i, 0)),
            smem,
        ],
        out_shape=[
            shape((4, heads, rows, D_HEAD), bf16),
            shape((4, heads, rows, D_HEAD), bf16),
            shape((2, rows, D_HEAD), f32),
            shape((16,), jnp.int32),
        ],
        name="prepare",
    )(queries, keys, values, out_grad, q_gain2, k_gain2, segments)
    got = lax.ppermute(theirs, "seq", swap_core)

    send = pl.pallas_call(
        functools.partial(pack_kernel, rows, heads),
        in_specs=[smem, vmem, vmem],
        out_specs=vmem,
        out_shape=shape((4, budget * UNIT, D_HEAD), bf16),
        name="pack",
    )(plan, mine, got)
    far = lax.ppermute(send, "seq", swap_chip)

    one_head = pl.BlockSpec((4, 1, rows, D_HEAD), lambda j: (0, j, 0, 0))
    seq_spec = pl.BlockSpec((1, seq), lambda j: (0, 0))
    gain_out = pl.BlockSpec((1, 2, D_HEAD), lambda j: (j, 0, 0))
    result_shapes = [
        shape((4, heads, rows, D_HEAD), bf16),
        shape((4, heads, rows, D_HEAD), bf16),
        shape((heads, 2, D_HEAD), f32),
    ]
    keep, give, gain_part = pl.pallas_call(
        functools.partial(local_kernel, rows),
        grid=(heads,),
        in_specs=[smem, one_head, one_head, seq_spec, seq_spec],
        out_specs=[one_head, one_head, gain_out],
        out_shape=result_shapes,
        scratch_shapes=[pltpu.VMEM((both, both), f32), pltpu.VMEM((both, D_HEAD), f32)],
        name="local",
    )(plan, mine, got, segments, visible)

    unit_spec = pl.BlockSpec((4, budget * UNIT, D_HEAD), lambda j: (0, 0, 0))
    keep, give, gain_part, back = pl.pallas_call(
        functools.partial(crossing_kernel, rows),
        grid=(heads,),
        in_specs=[smem, one_head, one_head, unit_spec, seq_spec, one_head, one_head, gain_out],
        out_specs=[one_head, one_head, gain_out, unit_spec],
        out_shape=result_shapes + [shape((4, budget * UNIT, D_HEAD), bf16)],
        scratch_shapes=[
            pltpu.VMEM((4, seq, D_HEAD), f32),
            pltpu.VMEM((4, seq, D_HEAD), f32),
            pltpu.VMEM((both, both), f32),
            pltpu.VMEM((8, D_HEAD), f32),
        ],
        name="crossing",
    )(plan, mine, got, far, visible, keep, give, gain_part)

    back = lax.ppermute(back, "seq", swap_chip)
    res_got = lax.ppermute(give, "seq", swap_core)
    total = gain_part
    step = 1
    while step < dp:
        total = total + lax.ppermute(total, "dp", [(i, i ^ step) for i in range(dp)])
        step *= 2
    total = total + lax.ppermute(total, "seq", swap_chip)
    total_got = lax.ppermute(total, "seq", swap_core)
    back_got = lax.ppermute(back, "seq", swap_core)

    full = shape((rows, width), bf16)
    attn_out, query_grad, key_grad, value_grad = pl.pallas_call(
        functools.partial(finish_kernel, rows, heads),
        in_specs=[smem] + [vmem] * 9,
        out_specs=[vmem] * 4,
        out_shape=[full] * 4,
        scratch_shapes=[pltpu.VMEM((rows, width), bf16), pltpu.VMEM((rows, width), bf16)],
        name="finish",
    )(plan, queries, keys, q_gain2, k_gain2, inv, keep, res_got, back, back_got)

    core = lax.rem(lax.axis_index("seq"), CORES)
    left = jnp.where(core == 0, total, total_got)
    right = jnp.where(core == 0, total_got, total)
    gains = jnp.concatenate([left, right], axis=0).transpose(1, 0, 2).reshape(2, width)
    return (attn_out, query_grad, key_grad, value_grad, gains[0] / q_gain, gains[1] / k_gain)


def solution(mesh):
    dp, seq = mesh.shape["dp"], mesh.shape["seq"]

    def per_device(queries, keys, values, q_gain, k_gain, out_grad, segments, visible):
        args = (queries, keys, values, q_gain, k_gain, out_grad, segments, visible)
        if seq == 2 * CORES and dp & (dp - 1) == 0:
            return per_device_clips(*args, dp)
        return per_device_any(*args)

    rows = P(("dp", "seq"), None)
    return jax.shard_map(
        per_device,
        mesh=mesh,
        in_specs=(rows, rows, rows, P(), P(), rows, P("dp", None), P("dp", None)),
        out_specs=(rows, rows, rows, rows, P(), P()),
        check_vma=False,
    )
```

```python
import functools

import jax
import jax.numpy as jnp
from jax import lax
from jax.experimental import pallas as pl
from jax.experimental.pallas import tpu as pltpu
from jax.sharding import PartitionSpec as P


D_HEAD = 128
UNIT = 16
CORES = 2
EPSILON = 1e-06
NEG = -1e30
PREPARE_STEPS = 2
LOCAL_GROUP = 4
CROSS_GROUPS = (2, 1)
FIRST_UNITS = 27


def normalize(raw_rows, gain_vec):
    raw_f32 = raw_rows.astype(jnp.float32)
    inv_rms = lax.rsqrt(jnp.mean(raw_f32 * raw_f32, axis=-1, keepdims=True) + EPSILON)
    return ((raw_f32 * inv_rms * gain_vec).astype(jnp.bfloat16), inv_rms)


def norm_back(raw_rows, inv_rms, gain_vec, grad_norm):
    raw_f32 = raw_rows.astype(jnp.float32)
    grad_f32 = grad_norm.astype(jnp.float32)
    scaled_grad = gain_vec * grad_f32
    mean_term = jnp.mean(scaled_grad * raw_f32, axis=-1, keepdims=True)
    grad_raw = inv_rms * scaled_grad - raw_f32 * inv_rms**3 * mean_term
    return (grad_raw.astype(jnp.bfloat16), jnp.sum(grad_f32 * raw_f32 * inv_rms, axis=0))


def attend(q_norm, k_norm, val_rows, grad_rows, seg_row, vis_row):
    seq_rows, feature_count = q_norm.shape
    heads = feature_count // D_HEAD
    scale = D_HEAD ** (-0.5)
    positions = jnp.arange(seq_rows, dtype=jnp.int32)
    allowed = (seg_row[:, None] == seg_row[None, :]) & (
        (vis_row[None, :] == 1) | (positions[:, None] == positions[None, :])
    )
    f32 = jnp.float32
    q, k, v, g = (
        x.reshape(seq_rows, heads, D_HEAD) for x in (q_norm, k_norm, val_rows, grad_rows)
    )
    scores = jnp.einsum("shd,thd->hst", q, k, preferred_element_type=f32) * scale
    scores = jnp.where(allowed[None], scores, NEG)
    weights = jnp.exp(scores - jnp.max(scores, axis=-1, keepdims=True))
    prob = weights / jnp.sum(weights, axis=-1, keepdims=True)
    half = prob.astype(jnp.bfloat16)
    out = jnp.einsum("hst,thd->shd", half, v, preferred_element_type=f32)
    dprob = jnp.einsum("shd,thd->hst", g, v, preferred_element_type=f32)
    v_grad = jnp.einsum("hst,shd->thd", half, g, preferred_element_type=f32)
    row_dot = jnp.sum(prob * dprob, axis=-1, keepdims=True)
    score_grad = (prob * (dprob - row_dot) * scale).astype(jnp.bfloat16)
    q_grad = jnp.einsum("hst,thd->shd", score_grad, k, preferred_element_type=f32)
    k_grad = jnp.einsum("hst,shd->thd", score_grad, q, preferred_element_type=f32)
    return tuple(
        x.reshape(seq_rows, feature_count).astype(jnp.bfloat16)
        for x in (out, q_grad, k_grad, v_grad)
    )


def per_device_any(queries, keys, values, q_gain, k_gain, out_grad, segments, visible):
    q_norm, q_inv = normalize(queries, q_gain)
    k_norm, k_inv = normalize(keys, k_gain)
    gather = functools.partial(
        lax.all_to_all, axis_name="seq", split_axis=1, concat_axis=0, tiled=True
    )
    spread = functools.partial(
        lax.all_to_all, axis_name="seq", split_axis=0, concat_axis=1, tiled=True
    )
    parts = attend(
        *(gather(x) for x in (q_norm, k_norm, values, out_grad)), segments[0], visible[0]
    )
    attn_out, q_grad, k_grad, value_grad = (spread(x) for x in parts)
    query_grad, q_gain_part = norm_back(queries, q_inv, q_gain, q_grad)
    key_grad, k_gain_part = norm_back(keys, k_inv, k_gain, k_grad)
    q_gain_grad, k_gain_grad = lax.psum((q_gain_part, k_gain_part), ("dp", "seq"))
    return (attn_out, query_grad, key_grad, value_grad, q_gain_grad, k_gain_grad)


def units_needed(blocks, heads):
    worst = 0
    for ka in range(1, blocks + 1):
        for kb in range(1, blocks + 2 - ka):
            worst = max(worst, min(max(ka * (heads - h), kb * h) for h in range(heads + 1)))
    return worst


def dot(x, y, dims):
    return lax.dot_general(x, y, (dims, ((), ())), preferred_element_type=jnp.float32)


NT = ((1,), (1,))
NN = ((1,), (0,))
TN = ((0,), (0,))
LOG2_E = 1.4426950408889634


def attention(q, k, v, g, bias):
    scale = D_HEAD ** (-0.5)
    scores = dot(k, q, NT) * (scale * LOG2_E) + bias
    weights = jnp.exp2(scores - jnp.max(scores, axis=0, keepdims=True))
    prob = weights * (1.0 / jnp.sum(weights, axis=0, keepdims=True))
    half = prob.astype(jnp.bfloat16)
    out = dot(half, v, TN)
    dprob = dot(v, g, NT)
    v_grad = dot(half, g, NN)
    row_dot = jnp.sum(prob * dprob, axis=0, keepdims=True)
    score_grad = (prob * scale * (dprob - row_dot)).astype(jnp.bfloat16)
    q_grad = dot(score_grad, k, TN)
    k_grad = dot(score_grad, q, NN)
    return tuple(x.astype(jnp.bfloat16) for x in (out, q_grad, k_grad, v_grad))


def own_side(plan):
    first = plan[0] == 0
    heads = plan[8]
    j0 = jnp.where(first, plan[6], 0)
    j1 = jnp.where(first, heads, plan[6])
    k_own = jnp.where(first, plan[4], plan[5])
    row0 = jnp.where(first, plan[9] - UNIT * plan[4], 0)
    return j0, j1, k_own, row0


def prepare_kernel(rows, heads, budget, steps, q_hbm, k_hbm, v_hbm, g_hbm, qg_hbm, kg_hbm, seg_hbm,
                   mine_ref, theirs_ref, inv_ref, plan_ref, q_ref, k_ref, qg_ref, kg_ref, seg_ref,
                   sems, head_sems):
    core = lax.rem(lax.axis_index("seq"), CORES)
    part = rows // steps

    def fetch(n, source, target):
        copy = pltpu.make_async_copy(source, target, sems.at[n])
        copy.start()
        return copy

    seg_copy = fetch(0, seg_hbm, seg_ref)
    gain_copies = [fetch(1, qg_hbm, qg_ref), fetch(2, kg_hbm, kg_ref)]
    raw_copies = []
    for n, (source, target) in enumerate(((q_hbm, q_ref), (k_hbm, k_ref))):
        for step in range(steps):
            here = pl.ds(step * part, part)
            raw_copies.append(fetch(3 + n * steps + step, source.at[here], target.at[here]))
    head_copies = []
    for n, source in ((2, v_hbm), (3, g_hbm)):
        for half, target in ((core, mine_ref), (1 - core, theirs_ref)):
            for j in range(heads):
                col = pl.ds(pl.multiple_of((half * heads + j) * D_HEAD, D_HEAD), D_HEAD)
                copy = pltpu.make_async_copy(
                    source.at[:, col], target.at[n, j], head_sems.at[len(head_copies)]
                )
                copy.start()
                head_copies.append(copy)

    seg_copy.wait()
    seg = seg_ref[...].astype(jnp.float32)
    chip_rows = seg.shape[1] // 2
    at = lax.broadcasted_iota(jnp.int32, seg.shape, 1)
    edge = jnp.sum(jnp.where(at == chip_rows - 1, seg, 0.0))
    beyond = jnp.sum(jnp.where(at == chip_rows, seg, 0.0))
    crosses = edge == beyond
    same = seg == edge
    a = jnp.sum(jnp.where(same & (at < chip_rows), 1.0, 0.0)).astype(jnp.int32)
    b = jnp.sum(jnp.where(same & (at >= chip_rows), 1.0, 0.0)).astype(jnp.int32)
    a = jnp.where(crosses, a, 0)
    b = jnp.where(crosses, b, 0)
    ka = lax.div(a + UNIT - 1, UNIT)
    kb = lax.div(b + UNIT - 1, UNIT)
    least = jnp.int32(0)
    most = jnp.int32(0)
    for h in range(heads):
        least += (ka * (heads - h) > budget).astype(jnp.int32)
        most += (kb * (h + 1) <= budget).astype(jnp.int32)
    plan_ref[0] = lax.div(lax.axis_index("seq"), CORES)
    plan_ref[1] = core
    plan_ref[2] = a
    plan_ref[3] = b
    plan_ref[4] = ka
    plan_ref[5] = kb
    plan_ref[6] = jnp.minimum(jnp.maximum(heads // 2, least), most)
    plan_ref[7] = crosses.astype(jnp.int32)
    plan_ref[8] = jnp.int32(heads)
    plan_ref[9] = jnp.int32(chip_rows)

    for copy in gain_copies:
        copy.wait()
    for n, (raw_ref, gain_ref) in enumerate(((q_ref, qg_ref), (k_ref, kg_ref))):
        for step in range(steps):
            raw_copies[n * steps + step].wait()
            here = pl.ds(step * part, part)
            raw = raw_ref[here, :].astype(jnp.float32)
            inv = lax.rsqrt(jnp.mean(raw * raw, axis=-1, keepdims=True) + EPSILON)
            inv_ref[n, here, :] = jnp.broadcast_to(inv, (part, D_HEAD))
            normed = (raw * inv * gain_ref[...]).astype(jnp.bfloat16)
            pieces = [normed[:, j * D_HEAD : (j + 1) * D_HEAD] for j in range(2 * heads)]

            @pl.when(core == 0)
            def _():
                for j in range(heads):
                    mine_ref[n, j, here, :] = pieces[j]
                    theirs_ref[n, j, here, :] = pieces[heads + j]

            @pl.when(core == 1)
            def _():
                for j in range(heads):
                    mine_ref[n, j, here, :] = pieces[heads + j]
                    theirs_ref[n, j, here, :] = pieces[j]

    for copy in head_copies:
        copy.wait()


def pack_kernel(rows, plan, mine_ref, got_ref, *send_refs):
    core = plan[1]
    j0, j1, k_own, row0 = own_side(plan)
    first_units = send_refs[0].shape[1] // UNIT
    for ref, half in ((mine_ref, core), (got_ref, 1 - core)):
        base = half * rows
        low = jnp.clip(lax.div(base - row0, UNIT), 0, k_own)
        high = jnp.clip(lax.div(base + rows - row0, UNIT), 0, k_own)

        def one_head(j, _, ref=ref, base=base, low=low, high=high):
            start = (j - j0) * k_own
            cut = jnp.clip(first_units - start, low, high)

            def unit_into(send_ref, shift):
                def one_unit(i, _):
                    at = pl.multiple_of(row0 + UNIT * i - base, UNIT)
                    to = pl.multiple_of((start + i - shift) * UNIT, UNIT)
                    for n in range(4):
                        send_ref[n, pl.ds(to, UNIT), :] = ref[n, j, pl.ds(at, UNIT), :]
                    return 0

                return one_unit

            lax.fori_loop(low, cut, unit_into(send_refs[0], 0), 0)
            if len(send_refs) > 1:
                lax.fori_loop(cut, high, unit_into(send_refs[1], first_units), 0)
            return 0

        lax.fori_loop(j0, j1, one_head, 0)


def local_kernel(rows, heads, group, plan, mine_ref, got_ref, seg_ref, vis_ref, qg_ref, kg_ref,
                 keep_ref, give_ref, gain_ref, cross_bias_ref, bias_ref, ok_ref):
    both = 2 * rows
    core, first = plan[1], plan[0] * both

    def chip_row(ref):
        wide = ref[...].astype(jnp.float32)
        total = wide.shape[1]
        wide = jnp.broadcast_to(wide, (8, total))
        own = pltpu.roll(wide, lax.rem(2 * total - first - core * rows, total), 1)
        other = pltpu.roll(wide, lax.rem(2 * total - first - (1 - core) * rows, total), 1)
        return jnp.concatenate([own[:, :rows], other[:, :rows]], axis=1)[0:1]

    seg = jnp.broadcast_to(chip_row(seg_ref), (both, both))
    code = jnp.broadcast_to(chip_row(seg_ref) * 2.0 + chip_row(vis_ref), (both, both))
    code_t = jnp.transpose(code)
    i = lax.broadcasted_iota(jnp.int32, (both, both), 0)
    j = lax.broadcasted_iota(jnp.int32, (both, both), 1)
    gap = code_t - 2.0 * seg
    allowed = (gap == 1.0) | (i == j)
    bias_ref[...] = jnp.where(allowed, 0.0, NEG)
    r = lax.broadcasted_iota(jnp.int32, (both, D_HEAD), 0)
    at = jnp.where(r < rows, core * rows + r, (1 - core) * rows + r - rows) + first
    edge = plan[9]
    crossing = (at >= edge - plan[2]) & (at < edge + plan[3])
    ok_ref[...] = jnp.where(crossing, 0.0, 1.0)
    wide = vis_ref[...].astype(jnp.float32)
    total = wide.shape[1]
    vis = pltpu.roll(jnp.broadcast_to(wide, (8, total)), lax.rem(total - edge + plan[2], total), 1)
    vis = jnp.transpose(jnp.broadcast_to(vis[0:1, :both], (both, both))) > 0.5
    length = plan[2] + plan[3]
    allowed = (i == j) | ((i < length) & (j < length) & vis)
    cross_bias_ref[...] = jnp.where(allowed, 0.0, NEG)

    def some_heads(step, _):
        for h in range(group):
            j = step * group + h
            q, k, v, g = (
                jnp.concatenate([mine_ref[n, j], got_ref[n, j]], axis=0) for n in range(4)
            )
            results = attention(q, k, v, g, bias_ref[...])
            for n, x in enumerate(results):
                keep_ref[n, j] = x[:rows]
                give_ref[n, j] = x[rows:]
            col = pl.ds(pl.multiple_of((core * heads + j) * D_HEAD, D_HEAD), D_HEAD)
            ok = ok_ref[...]
            for n, (x, y, gain) in enumerate(
                ((q, results[1], qg_ref), (k, results[2], kg_ref))
            ):
                term = ok * x.astype(jnp.float32) * y.astype(jnp.float32)
                gain_ref[n, pl.ds(j, 1), :] = jnp.sum(term, axis=0, keepdims=True) / gain[:, col]
        return 0

    lax.fori_loop(0, heads // group, some_heads, 0)


def crossing_kernel(rows, heads, stage, stages, group, plan, mine_ref, got_ref, far_refs, bias_ref,
                    qg_ref, kg_ref, gain_in, keep_ref, give_ref, gain_ref, back_ref, seq_ref,
                    res_ref):
    both = 2 * rows
    chip, core = plan[0], plan[1]
    a, b = plan[2], plan[3]
    first = chip == 0
    edge = plan[9]
    start = edge - a
    own_lo = chip * both
    k_far = jnp.where(first, plan[5], plan[4])
    far_row0 = jnp.where(first, edge, edge - UNIT * plan[4])
    j0 = jnp.where(first, 0, plan[6])
    count = jnp.where(plan[7] == 1, jnp.where(first, plan[6], heads - plan[6]), 0)
    first_units = far_refs[0].shape[1] // UNIT
    if stages == 1:
        low, high = 0, count
    else:
        ready = jnp.minimum(lax.div(first_units, jnp.maximum(k_far, 1)), count)
        low, high = (0, ready) if stage == 0 else (ready, count)

    gain_ref[...] = gain_in[...]
    own_at = pl.multiple_of(own_lo + core * rows, rows)
    got_at = pl.multiple_of(own_lo + (1 - core) * rows, rows)

    def some_heads(step, _):
        places = [jnp.minimum(low + step * group + s, high - 1) for s in range(group)]
        for s, jj in enumerate(places):
            j = j0 + jj
            for n in range(4):
                seq_ref[s, n, pl.ds(own_at, rows), :] = mine_ref[n, j].astype(jnp.float32)
                seq_ref[s, n, pl.ds(got_at, rows), :] = got_ref[n, j].astype(jnp.float32)

            def load_from(far_ref, shift, s=s, jj=jj):
                def load(i, _):
                    at = pl.multiple_of((jj * k_far + i - shift) * UNIT, UNIT)
                    to = pl.multiple_of(far_row0 + UNIT * i, UNIT)
                    for n in range(4):
                        seq_ref[s, n, pl.ds(to, UNIT), :] = far_ref[n, pl.ds(at, UNIT), :].astype(
                            jnp.float32
                        )
                    return 0

                return load

            if stage == 0:
                lax.fori_loop(0, k_far, load_from(far_refs[0], 0), 0)
            else:
                cut = jnp.clip(first_units - jj * k_far, 0, k_far)
                lax.fori_loop(0, cut, load_from(far_refs[0], 0), 0)
                lax.fori_loop(cut, k_far, load_from(far_refs[1], first_units), 0)
        for s, jj in enumerate(places):
            j = j0 + jj
            inside = lax.broadcasted_iota(jnp.int32, (both, D_HEAD), 0) < a + b
            q, k, v, g = (
                jnp.where(inside, seq_ref[s, n, pl.ds(start, both), :], 0.0).astype(jnp.bfloat16)
                for n in range(4)
            )
            results = attention(q, k, v, g, bias_ref[...])
            for n, x in enumerate(results):
                res_ref[s, n, pl.ds(start, both), :] = x.astype(jnp.float32)
            col = pl.ds(pl.multiple_of((core * heads + j) * D_HEAD, D_HEAD), D_HEAD)
            for n, (x, y, gain) in enumerate(
                ((q, results[1], qg_ref), (k, results[2], kg_ref))
            ):
                term = x.astype(jnp.float32) * y.astype(jnp.float32)
                gain_ref[n, pl.ds(j, 1), :] = (
                    gain_in[n, pl.ds(j, 1), :] + jnp.sum(term, axis=0, keepdims=True) / gain[:, col]
                )
        for s, jj in enumerate(places):
            j = j0 + jj
            r = lax.broadcasted_iota(jnp.int32, (rows, D_HEAD), 0)
            for at, ref in ((own_at, keep_ref), (got_at, give_ref)):
                inside = (r + at >= start) & (r + at < edge + b)
                for n in range(4):
                    x = res_ref[s, n, pl.ds(at, rows), :]
                    old = ref[n, j].astype(jnp.float32)
                    ref[n, j] = jnp.where(inside, x, old).astype(jnp.bfloat16)

            def store(i, _, s=s, jj=jj):
                to = pl.multiple_of((jj * k_far + i) * UNIT, UNIT)
                at = pl.multiple_of(far_row0 + UNIT * i, UNIT)
                for n in range(4):
                    back_ref[n, pl.ds(to, UNIT), :] = res_ref[s, n, pl.ds(at, UNIT), :].astype(
                        jnp.bfloat16
                    )
                return 0

            lax.fori_loop(0, k_far, store, 0)
        return 0

    lax.fori_loop(0, lax.div(high - low + group - 1, group), some_heads, 0)


def assemble_kernel(heads, plan, keep_ref, got_ref, *to_refs):
    core = plan[1]
    for ref, side in ((keep_ref, core), (got_ref, 1 - core)):
        for j in range(heads):
            col = pl.multiple_of((side * heads + j) * D_HEAD, D_HEAD)
            for n in range(4):
                to_refs[n][:, pl.ds(col, D_HEAD)] = ref[n, j]


def join_kernel(heads, plan, own_ref, got_ref, to_ref):
    to_ref[:, pl.ds(pl.multiple_of(plan[1] * heads, heads), heads), :] = own_ref[...]
    to_ref[:, pl.ds(pl.multiple_of((1 - plan[1]) * heads, heads), heads), :] = got_ref[...]


def add_kernel(x_ref, y_ref, to_ref):
    to_ref[...] = x_ref[...] + y_ref[...]


def finish_kernel(rows, heads, plan, q_ref, k_ref, qg_ref, kg_ref, inv_ref, back_ref,
                  back_got_ref, *rest):
    out_hbm, dq_hbm, dk_hbm, dv_hbm, *held = rest[4:12]
    wide_ref, dq_ref, dk_ref, sems = rest[12:]
    core = plan[1]
    j0, j1, k_own, row0 = own_side(plan)
    base = core * rows
    length = back_ref.shape[1]
    for s, ref in enumerate((back_ref, back_got_ref)):
        wide_ref[s, :, pl.ds(rows, length), :] = ref[...]
    r = lax.broadcasted_iota(jnp.int32, (rows, D_HEAD), 0) + base
    first = plan[0] == 0
    inside = (r >= jnp.where(first, plan[9] - plan[2], 0)) & (
        r < jnp.where(first, plan[9], plan[3])
    )

    def one_head(j, _):
        at = (j - j0) * k_own * UNIT + base - row0 + rows
        at = pl.multiple_of(jnp.clip(at, 0, length + rows), UNIT)
        for s, side in ((0, core), (1, 1 - core)):
            col = pl.multiple_of((side * heads + j) * D_HEAD, D_HEAD)
            for n in range(4):
                new = wide_ref[s, n, pl.ds(at, rows), :].astype(jnp.float32)
                old = held[n][:, pl.ds(col, D_HEAD)].astype(jnp.float32)
                held[n][:, pl.ds(col, D_HEAD)] = jnp.where(inside, new, old).astype(jnp.bfloat16)
        return 0

    lax.fori_loop(j0, jnp.where(k_own > 0, j1, j0), one_head, 0)
    copies = [
        pltpu.make_async_copy(held[0], out_hbm, sems.at[0]),
        pltpu.make_async_copy(held[3], dv_hbm, sems.at[1]),
        pltpu.make_async_copy(dq_ref, dq_hbm, sems.at[2]),
        pltpu.make_async_copy(dk_ref, dk_hbm, sems.at[3]),
    ]
    copies[0].start()
    copies[1].start()
    for n, (raw_ref, gain_ref, grad_ref, to_ref) in enumerate(
        ((q_ref, qg_ref, held[1], dq_ref), (k_ref, kg_ref, held[2], dk_ref))
    ):
        raw = raw_ref[...].astype(jnp.float32)
        scaled = gain_ref[...] * grad_ref[...].astype(jnp.float32)
        mean_term = jnp.mean(scaled * raw, axis=-1, keepdims=True)
        inv = inv_ref[n, :, 0:1]
        to_ref[...] = (inv * scaled - raw * (inv * inv * inv * mean_term)).astype(jnp.bfloat16)
        copies[2 + n].start()
    for copy in copies:
        copy.wait()


def per_device_clips(queries, keys, values, q_gain, k_gain, out_grad, segments, visible, dp):
    rows, width = queries.shape
    heads = width // D_HEAD // CORES
    seq = segments.shape[1]
    budget = units_needed(CORES * rows // UNIT, heads)
    both = CORES * rows
    bf16, f32 = jnp.bfloat16, jnp.float32
    smem = pl.BlockSpec(memory_space=pltpu.SMEM)
    vmem = pl.BlockSpec(memory_space=pltpu.VMEM)
    hbm = pl.BlockSpec(memory_space=pl.ANY)
    limit = lambda mib: pltpu.CompilerParams(vmem_limit_bytes=mib << 20)
    keep_in_vmem = lambda x: pltpu.with_memory_space_constraint(x, pltpu.VMEM)
    swap_core = [(i, i ^ 1) for i in range(4)]
    swap_chip = [(i, i ^ 2) for i in range(4)]
    q_gain2, k_gain2 = q_gain[None], k_gain[None]
    split = pltpu.VMEM((4, heads, rows, D_HEAD), bf16)

    hbm_only = pl.BlockSpec(memory_space=pltpu.HBM)
    mine, theirs, inv, plan = pl.pallas_call(
        functools.partial(prepare_kernel, rows, heads, budget, PREPARE_STEPS),
        in_specs=[hbm_only] * 7,
        out_specs=[vmem, vmem, vmem, smem],
        out_shape=[
            split,
            split,
            pltpu.VMEM((2, rows, D_HEAD), f32),
            jax.ShapeDtypeStruct((16,), jnp.int32),
        ],
        scratch_shapes=[
            pltpu.VMEM((rows, width), bf16),
            pltpu.VMEM((rows, width), bf16),
            pltpu.VMEM((1, width), f32),
            pltpu.VMEM((1, width), f32),
            pltpu.VMEM((1, seq), jnp.int32),
            pltpu.SemaphoreType.DMA((3 + 2 * PREPARE_STEPS,)),
            pltpu.SemaphoreType.DMA((4 * heads,)),
        ],
        compiler_params=limit(16),
        name="prepare",
    )(*[pltpu.with_memory_space_constraint(x, pltpu.HBM)
        for x in (queries, keys, values, out_grad, q_gain2, k_gain2, segments)])
    got = keep_in_vmem(lax.ppermute(theirs, "seq", swap_core))
    mine = keep_in_vmem(mine)

    sizes = [budget] if FIRST_UNITS is None else [FIRST_UNITS, budget - FIRST_UNITS]
    sends = pl.pallas_call(
        functools.partial(pack_kernel, rows),
        in_specs=[smem, vmem, vmem],
        out_specs=[vmem] * len(sizes),
        out_shape=[pltpu.VMEM((4, n * UNIT, D_HEAD), bf16) for n in sizes],
        compiler_params=limit(4),
        name="pack",
    )(plan, mine, got)
    fars = [keep_in_vmem(lax.ppermute(x, "seq", swap_chip)) for x in sends]

    gains_shape = pltpu.VMEM((2, heads, D_HEAD), f32)
    keep, give, gain_part, cross_bias = pl.pallas_call(
        functools.partial(local_kernel, rows, heads, LOCAL_GROUP),
        in_specs=[smem] + [vmem] * 6,
        out_specs=[vmem] * 4,
        out_shape=[split, split, gains_shape, pltpu.VMEM((both, both), f32)],
        scratch_shapes=[pltpu.VMEM((both, both), f32), pltpu.VMEM((both, D_HEAD), f32)],
        compiler_params=limit(16),
        name="local",
    )(plan, mine, got, segments, visible, q_gain2, k_gain2)

    back_shape = pltpu.VMEM((4, budget * UNIT, D_HEAD), bf16)
    back = None
    for stage in range(len(sizes)):
        args = [plan, mine, got, *fars[: stage + 1], keep_in_vmem(cross_bias), q_gain2, k_gain2]
        args += [keep_in_vmem(x) for x in (gain_part, keep, give)]
        aliases = {len(args) - 2: 0, len(args) - 1: 1}
        if stage:
            aliases[len(args)] = 3
            args.append(keep_in_vmem(back))

        def body(*refs, stage=stage, count=len(args)):
            ins, outs = refs[:count], refs[count:]
            far = ins[3 : 4 + stage]
            vis, qg, kg, gain_in = ins[4 + stage : 8 + stage]
            crossing_kernel(rows, heads, stage, len(sizes), CROSS_GROUPS[stage], ins[0], ins[1], ins[2],
                            far, vis, qg, kg, gain_in, *outs)

        keep, give, gain_part, back = pl.pallas_call(
            body,
            in_specs=[smem] + [vmem] * (len(args) - 1),
            out_specs=[vmem] * 4,
            out_shape=[split, split, gains_shape, back_shape],
            input_output_aliases=aliases,
            scratch_shapes=[
                pltpu.VMEM((CROSS_GROUPS[stage], 4, seq, D_HEAD), f32),
                pltpu.VMEM((CROSS_GROUPS[stage], 4, seq, D_HEAD), f32),
            ],
            compiler_params=limit(20),
        )(*args)

    back = lax.ppermute(back, "seq", swap_chip)
    res_got = keep_in_vmem(lax.ppermute(give, "seq", swap_core))
    gain_got = lax.ppermute(gain_part, "seq", swap_core)
    total_shape = pltpu.VMEM((2, CORES * heads, D_HEAD), f32)
    total = pl.pallas_call(
        functools.partial(join_kernel, heads),
        in_specs=[smem, vmem, vmem],
        out_specs=vmem,
        out_shape=total_shape,
        compiler_params=limit(1),
        name="join",
    )(plan, keep_in_vmem(gain_part), keep_in_vmem(gain_got))
    step = 1
    while step < dp:
        total_got = lax.ppermute(total, "dp", [(i, i ^ step) for i in range(dp)])
        total = pl.pallas_call(
            add_kernel,
            in_specs=[vmem, vmem],
            out_specs=vmem,
            out_shape=total_shape,
            compiler_params=limit(1),
            name="add",
        )(keep_in_vmem(total), keep_in_vmem(total_got))
        step *= 2

    held = pl.pallas_call(
        functools.partial(assemble_kernel, heads),
        in_specs=[smem, vmem, vmem],
        out_specs=[vmem] * 4,
        out_shape=[pltpu.VMEM((rows, width), bf16)] * 4,
        compiler_params=limit(4),
        name="assemble",
    )(plan, keep_in_vmem(keep), res_got)

    back, total, held = lax.optimization_barrier((back, total, held))
    back_got = keep_in_vmem(lax.ppermute(back, "seq", swap_core))
    total_got = lax.ppermute(total, "seq", swap_chip)

    full = jax.ShapeDtypeStruct((rows, width), bf16)
    outs = pl.pallas_call(
        functools.partial(finish_kernel, rows, heads),
        in_specs=[smem] + [vmem] * 11,
        out_specs=[hbm] * 4 + [vmem] * 4,
        out_shape=[full] * 4 + [pltpu.VMEM((rows, width), bf16)] * 4,
        input_output_aliases={8 + i: 4 + i for i in range(4)},
        scratch_shapes=[
            pltpu.VMEM((2, 4, budget * UNIT + 2 * rows, D_HEAD), bf16),
            pltpu.VMEM((rows, width), bf16),
            pltpu.VMEM((rows, width), bf16),
            pltpu.SemaphoreType.DMA((4,)),
        ],
        compiler_params=limit(12),
        name="finish",
    )(plan, keep_in_vmem(queries), keep_in_vmem(keys), q_gain2, k_gain2, keep_in_vmem(inv), keep_in_vmem(back), back_got,
      *[keep_in_vmem(x) for x in held])
    attn_out, query_grad, key_grad, value_grad = outs[:4]
    total = total + total_got
    return (attn_out, query_grad, key_grad, value_grad, total[0].reshape(width), total[1].reshape(width))


def solution(mesh):
    dp, seq = mesh.shape["dp"], mesh.shape["seq"]
    two_chips = seq == 2 * CORES and dp & (dp - 1) == 0

    def per_device(queries, keys, values, q_gain, k_gain, out_grad, segments, visible):
        args = (queries, keys, values, q_gain, k_gain, out_grad, segments, visible)
        if two_chips:
            return per_device_clips(*args, dp)
        return per_device_any(*args)

    rows = P(("dp", "seq"), None)
    return jax.shard_map(
        per_device,
        mesh=mesh,
        in_specs=(rows, rows, rows, P(), P(), rows, P("dp", None), P("dp", None)),
        out_specs=(rows, rows, rows, rows, P(), P()),
        check_vma=False,
    )
```

```python
import functools

import jax
import jax.numpy as jnp
from jax import lax
from jax.experimental import pallas as pl
from jax.experimental.pallas import tpu as pltpu
from jax.sharding import PartitionSpec as P


D_HEAD = 128
UNIT = 16
CORES = 2
EPSILON = 1e-06
NEG = -1e30
LOCAL_GROUP = 4
CROSS_GROUP = 2
PARTS = (2, 3)


def normalize(raw_rows, gain_vec):
    raw_f32 = raw_rows.astype(jnp.float32)
    inv_rms = lax.rsqrt(jnp.mean(raw_f32 * raw_f32, axis=-1, keepdims=True) + EPSILON)
    return ((raw_f32 * inv_rms * gain_vec).astype(jnp.bfloat16), inv_rms)


def norm_back(raw_rows, inv_rms, gain_vec, grad_norm):
    raw_f32 = raw_rows.astype(jnp.float32)
    grad_f32 = grad_norm.astype(jnp.float32)
    scaled_grad = gain_vec * grad_f32
    mean_term = jnp.mean(scaled_grad * raw_f32, axis=-1, keepdims=True)
    grad_raw = inv_rms * scaled_grad - raw_f32 * inv_rms**3 * mean_term
    return (grad_raw.astype(jnp.bfloat16), jnp.sum(grad_f32 * raw_f32 * inv_rms, axis=0))


def attend(q_norm, k_norm, val_rows, grad_rows, seg_row, vis_row):
    seq_rows, feature_count = q_norm.shape
    heads = feature_count // D_HEAD
    scale = D_HEAD ** (-0.5)
    positions = jnp.arange(seq_rows, dtype=jnp.int32)
    allowed = (seg_row[:, None] == seg_row[None, :]) & (
        (vis_row[None, :] == 1) | (positions[:, None] == positions[None, :])
    )
    f32 = jnp.float32
    q, k, v, g = (
        x.reshape(seq_rows, heads, D_HEAD) for x in (q_norm, k_norm, val_rows, grad_rows)
    )
    scores = jnp.einsum("shd,thd->hst", q, k, preferred_element_type=f32) * scale
    scores = jnp.where(allowed[None], scores, NEG)
    weights = jnp.exp(scores - jnp.max(scores, axis=-1, keepdims=True))
    prob = weights / jnp.sum(weights, axis=-1, keepdims=True)
    half = prob.astype(jnp.bfloat16)
    out = jnp.einsum("hst,thd->shd", half, v, preferred_element_type=f32)
    dprob = jnp.einsum("shd,thd->hst", g, v, preferred_element_type=f32)
    v_grad = jnp.einsum("hst,shd->thd", half, g, preferred_element_type=f32)
    row_dot = jnp.sum(prob * dprob, axis=-1, keepdims=True)
    score_grad = (prob * (dprob - row_dot) * scale).astype(jnp.bfloat16)
    q_grad = jnp.einsum("hst,thd->shd", score_grad, k, preferred_element_type=f32)
    k_grad = jnp.einsum("hst,shd->thd", score_grad, q, preferred_element_type=f32)
    return tuple(
        x.reshape(seq_rows, feature_count).astype(jnp.bfloat16)
        for x in (out, q_grad, k_grad, v_grad)
    )


def per_device_any(queries, keys, values, q_gain, k_gain, out_grad, segments, visible):
    q_norm, q_inv = normalize(queries, q_gain)
    k_norm, k_inv = normalize(keys, k_gain)
    gather = functools.partial(
        lax.all_to_all, axis_name="seq", split_axis=1, concat_axis=0, tiled=True
    )
    spread = functools.partial(
        lax.all_to_all, axis_name="seq", split_axis=0, concat_axis=1, tiled=True
    )
    parts = attend(
        *(gather(x) for x in (q_norm, k_norm, values, out_grad)), segments[0], visible[0]
    )
    attn_out, q_grad, k_grad, value_grad = (spread(x) for x in parts)
    query_grad, q_gain_part = norm_back(queries, q_inv, q_gain, q_grad)
    key_grad, k_gain_part = norm_back(keys, k_inv, k_gain, k_grad)
    q_gain_grad, k_gain_grad = lax.psum((q_gain_part, k_gain_part), ("dp", "seq"))
    return (attn_out, query_grad, key_grad, value_grad, q_gain_grad, k_gain_grad)


def units_needed(blocks, heads):
    worst = 0
    for ka in range(1, blocks + 1):
        for kb in range(1, blocks + 2 - ka):
            worst = max(worst, min(max(ka * (heads - h), kb * h) for h in range(heads + 1)))
    return worst


def dot(x, y, dims):
    return lax.dot_general(x, y, (dims, ((), ())), preferred_element_type=jnp.float32)


NT = ((1,), (1,))
NN = ((1,), (0,))
TN = ((0,), (0,))
LOG2_E = 1.4426950408889634


def attention(q, k, v, g, bias):
    scale = D_HEAD ** (-0.5)
    scores = dot(k, q, NT) * (scale * LOG2_E) + bias
    weights = jnp.exp2(scores - jnp.max(scores, axis=0, keepdims=True))
    prob = weights * (1.0 / jnp.sum(weights, axis=0, keepdims=True))
    half = prob.astype(jnp.bfloat16)
    out = dot(half, v, TN)
    dprob = dot(v, g, NT)
    v_grad = dot(half, g, NN)
    row_dot = jnp.sum(prob * dprob, axis=0, keepdims=True)
    score_grad = (prob * scale * (dprob - row_dot)).astype(jnp.bfloat16)
    q_grad = dot(score_grad, k, TN)
    k_grad = dot(score_grad, q, NN)
    return tuple(x.astype(jnp.bfloat16) for x in (out, q_grad, k_grad, v_grad))


def own_side(plan):
    first = plan[0] == 0
    heads = plan[8]
    j0 = jnp.where(first, plan[6], 0)
    j1 = jnp.where(first, heads, plan[6])
    k_own = jnp.where(first, plan[4], plan[5])
    row0 = jnp.where(first, plan[9] - UNIT * plan[4], 0)
    return j0, j1, k_own, row0


def fetch_kernel(heads, budget, q_hbm, k_hbm, v_hbm, g_hbm, seg_hbm, mine_ref, theirs_ref,
                 q_ref, k_ref, plan_ref, seg_ref, sems, head_sems):
    core = lax.rem(lax.axis_index("seq"), CORES)

    def fetch(source, target, sem):
        copy = pltpu.make_async_copy(source, target, sem)
        copy.start()
        return copy

    seg_copy = fetch(seg_hbm, seg_ref, sems.at[0])
    copies = []
    for half, target in ((1 - core, theirs_ref), (core, mine_ref)):
        for n, source in enumerate((v_hbm, g_hbm)):
            for j in range(heads):
                col = pl.ds(pl.multiple_of((half * heads + j) * D_HEAD, D_HEAD), D_HEAD)
                copies.append(fetch(source.at[:, col], target.at[n, j], head_sems.at[len(copies)]))
    copies.append(fetch(q_hbm, q_ref, sems.at[1]))
    copies.append(fetch(k_hbm, k_ref, sems.at[2]))

    seg_copy.wait()
    seg = seg_ref[...].astype(jnp.float32)
    chip_rows = seg.shape[1] // 2
    at = lax.broadcasted_iota(jnp.int32, seg.shape, 1)
    edge = jnp.sum(jnp.where(at == chip_rows - 1, seg, 0.0))
    beyond = jnp.sum(jnp.where(at == chip_rows, seg, 0.0))
    crosses = edge == beyond
    same = seg == edge
    a = jnp.sum(jnp.where(same & (at < chip_rows), 1.0, 0.0)).astype(jnp.int32)
    b = jnp.sum(jnp.where(same & (at >= chip_rows), 1.0, 0.0)).astype(jnp.int32)
    a = jnp.where(crosses, a, 0)
    b = jnp.where(crosses, b, 0)
    ka = lax.div(a + UNIT - 1, UNIT)
    kb = lax.div(b + UNIT - 1, UNIT)
    least = jnp.int32(0)
    most = jnp.int32(0)
    for h in range(heads):
        least += (ka * (heads - h) > budget).astype(jnp.int32)
        most += (kb * (h + 1) <= budget).astype(jnp.int32)
    plan_ref[0] = lax.div(lax.axis_index("seq"), CORES)
    plan_ref[1] = core
    plan_ref[2] = a
    plan_ref[3] = b
    plan_ref[4] = ka
    plan_ref[5] = kb
    plan_ref[6] = jnp.minimum(jnp.maximum(heads // 2, least), most)
    plan_ref[7] = crosses.astype(jnp.int32)
    plan_ref[8] = jnp.int32(heads)
    plan_ref[9] = jnp.int32(chip_rows)

    for copy in copies:
        copy.wait()


def prepare_kernel(rows, heads, plan, q_ref, k_ref, qg_ref, kg_ref, mine_ref, theirs_ref, inv_ref):
    for n, (raw_ref, gain_ref) in enumerate(((q_ref, qg_ref), (k_ref, kg_ref))):
        raw = raw_ref[...].astype(jnp.float32)
        inv = lax.rsqrt(jnp.mean(raw * raw, axis=-1, keepdims=True) + EPSILON)
        inv_ref[n] = jnp.broadcast_to(inv, (rows, D_HEAD))
        normed = (raw * inv * gain_ref[...]).astype(jnp.bfloat16)
        pieces = [normed[:, j * D_HEAD : (j + 1) * D_HEAD] for j in range(2 * heads)]

        @pl.when(plan[1] == 0)
        def _():
            for j in range(heads):
                mine_ref[n, j] = pieces[j]
                theirs_ref[n, j] = pieces[heads + j]

        @pl.when(plan[1] == 1)
        def _():
            for j in range(heads):
                mine_ref[n, j] = pieces[heads + j]
                theirs_ref[n, j] = pieces[j]


def pack_kernel(rows, plan, mine_ref, got_ref, *send_refs):
    core = plan[1]
    j0, j1, k_own, row0 = own_side(plan)
    for ref, half in ((mine_ref, core), (got_ref, 1 - core)):
        base = half * rows
        low = jnp.clip(lax.div(base - row0, UNIT), 0, k_own)
        high = jnp.clip(lax.div(base + rows - row0, UNIT), 0, k_own)

        def one_head(j, _, ref=ref, base=base, low=low, high=high):
            start = (j - j0) * k_own

            def unit_into(send_ref, shift):
                def one_unit(i, _):
                    at = pl.multiple_of(row0 + UNIT * i - base, UNIT)
                    to = pl.multiple_of((start + i - shift) * UNIT, UNIT)
                    for n in range(2):
                        send_ref[n, pl.ds(to, UNIT), :] = ref[n, j, pl.ds(at, UNIT), :]
                    return 0

                return one_unit

            shift, done = 0, low
            for n, send_ref in enumerate(send_refs):
                units = send_ref.shape[1] // UNIT
                last = n == len(send_refs) - 1
                cut = high if last else jnp.clip(shift + units - start, low, high)
                lax.fori_loop(done, cut, unit_into(send_ref, shift), 0)
                shift, done = shift + units, cut
            return 0

        lax.fori_loop(j0, j1, one_head, 0)


def local_kernel(rows, heads, group, plan, mine_qk, mine_vg, got_qk, got_vg, seg_ref, vis_ref, qg_ref, kg_ref,
                 keep_ref, give_ref, gain_ref, cross_bias_ref, place_ref, bias_ref, ok_ref):
    both = 2 * rows
    core, first = plan[1], plan[0] * both
    mine = [mine_qk.at[0], mine_qk.at[1], mine_vg.at[0], mine_vg.at[1]]
    got = [got_qk.at[0], got_qk.at[1], got_vg.at[0], got_vg.at[1]]

    def chip_row(ref):
        wide = ref[...].astype(jnp.float32)
        total = wide.shape[1]
        wide = jnp.broadcast_to(wide, (8, total))
        own = pltpu.roll(wide, lax.rem(2 * total - first - core * rows, total), 1)
        other = pltpu.roll(wide, lax.rem(2 * total - first - (1 - core) * rows, total), 1)
        return jnp.concatenate([own[:, :rows], other[:, :rows]], axis=1)[0:1]

    seg = jnp.broadcast_to(chip_row(seg_ref), (both, both))
    code = jnp.broadcast_to(chip_row(seg_ref) * 2.0 + chip_row(vis_ref), (both, both))
    code_t = jnp.transpose(code)
    i = lax.broadcasted_iota(jnp.int32, (both, both), 0)
    j = lax.broadcasted_iota(jnp.int32, (both, both), 1)
    gap = code_t - 2.0 * seg
    allowed = (gap == 1.0) | (i == j)
    bias_ref[...] = jnp.where(allowed, 0.0, NEG)
    r = lax.broadcasted_iota(jnp.int32, (both, D_HEAD), 0)
    at = jnp.where(r < rows, core * rows + r, (1 - core) * rows + r - rows) + first
    edge = plan[9]
    crossing = (at >= edge - plan[2]) & (at < edge + plan[3])
    ok_ref[...] = jnp.where(crossing, 0.0, 1.0)
    wide = jnp.broadcast_to(vis_ref[...].astype(jnp.float32), (8, 2 * both))
    in_first, in_last = j >= both - plan[2], j < plan[3]
    vis = jnp.where(in_first[:8], wide[:, :both], wide[:, both:])
    vis = jnp.broadcast_to(vis[0:1], (both, both)) > 0.5
    in_clip = (in_first | in_last) & ((i >= both - plan[2]) | (i < plan[3]))
    allowed = jnp.transpose(jnp.where(in_clip & vis, 1.0, 0.0)) > 0.5
    cross_bias_ref[...] = jnp.where(allowed | (i == j), 0.0, NEG)
    low, high = r < plan[3], r >= both - plan[2]
    is_first = (r >= 0) & (plan[0] == 0)
    from_own = jnp.where(is_first, jnp.where(high, 1.0, 0.0), jnp.where(low, 1.0, 0.0))
    from_far = jnp.where(is_first, jnp.where(low, 1.0, 0.0), jnp.where(high, 1.0, 0.0))
    place_ref[0] = from_own.astype(jnp.bfloat16)
    place_ref[1] = from_far.astype(jnp.bfloat16)

    def some_heads(step, _):
        for h in range(group):
            j = step * group + h
            q, k, v, g = (
                jnp.concatenate([mine[n][j], got[n][j]], axis=0) for n in range(4)
            )
            results = attention(q, k, v, g, bias_ref[...])
            for n, x in enumerate(results):
                keep_ref[n, j] = x[:rows]
                give_ref[n, j] = x[rows:]
            col = pl.ds(pl.multiple_of((core * heads + j) * D_HEAD, D_HEAD), D_HEAD)
            ok = ok_ref[...]
            for n, (x, y, gain) in enumerate(
                ((q, results[1], qg_ref), (k, results[2], kg_ref))
            ):
                term = ok * x.astype(jnp.float32) * y.astype(jnp.float32)
                gain_ref[n, pl.ds(j, 1), :] = jnp.sum(term, axis=0, keepdims=True) / gain[:, col]
        return 0

    lax.fori_loop(0, heads // group, some_heads, 0)


def crossing_kernel(rows, heads, stage, stages, group, plan, mine_refs, got_refs, far_vg, far_refs, bias_ref,
                    place_ref, qg_ref, kg_ref, gain_in, keep_ref, give_ref, gain_ref, wide_back_ref,
                    back_refs, far_ref, res_ref):
    both = 2 * rows
    core, first = plan[1], plan[0] == 0
    k_far = jnp.where(first, plan[5], plan[4])
    j0 = jnp.where(first, 0, plan[6])
    count = jnp.where(plan[7] == 1, jnp.where(first, plan[6], heads - plan[6]), 0)
    units = [ref.shape[1] // UNIT for ref in far_refs]
    ready = lambda n: jnp.minimum(lax.div(n, jnp.maximum(k_far, 1)), count)
    low = ready(sum(units[:-1])) if stage else 0
    high = ready(sum(units)) if stage < stages - 1 else count

    @pl.when(high > low)
    def _():
        at = both
        for ref in far_refs:
            far_ref[0:2, pl.ds(at, ref.shape[1]), :] = ref[...]
            at += ref.shape[1]
        far_ref[2:4, pl.ds(both, far_vg.shape[1]), :] = far_vg[...]

    gain_ref[...] = gain_in[...]
    far_lo = jnp.where(first, both, UNIT * k_far)
    res_lo = pl.multiple_of(jnp.where(first, 0, both - UNIT * k_far), UNIT)

    def some_heads(jj_first, group):
        places = [jj_first + s for s in range(group)]
        from_own, from_far = place_ref[0] > 0.5, place_ref[1] > 0.5
        for s, jj in enumerate(places):
            j = j0 + jj
            far = pl.ds(pl.multiple_of(far_lo + UNIT * jj * k_far, UNIT), both)
            loaded = []
            for n in range(4):
                mine, got = mine_refs[n // 2][n % 2, j], got_refs[n // 2][n % 2, j]
                own = jnp.where(
                    core == 0,
                    jnp.concatenate([mine, got], axis=0),
                    jnp.concatenate([got, mine], axis=0),
                )
                distant = jnp.where(from_far, far_ref[n, far, :], jnp.zeros_like(own))
                loaded.append(jnp.where(from_own, own, distant))
            q, k, v, g = loaded
            results = attention(q, k, v, g, bias_ref[...])
            own_rows = pl.ds(pl.multiple_of(core * rows, rows), rows)
            got_rows = pl.ds(pl.multiple_of((1 - core) * rows, rows), rows)
            for n, x in enumerate(results):
                res_ref[s, n, pl.ds(0, both), :] = x
            for here, ref in ((own_rows, keep_ref), (got_rows, give_ref)):
                ours = place_ref[0, here, :] > 0.5
                for n in range(4):
                    ref[n, j] = jnp.where(ours, res_ref[s, n, here, :], ref[n, j])
            col = pl.ds(pl.multiple_of((core * heads + j) * D_HEAD, D_HEAD), D_HEAD)
            for n, (x, y, gain) in enumerate(
                ((q, results[1], qg_ref), (k, results[2], kg_ref))
            ):
                term = x.astype(jnp.float32) * y.astype(jnp.float32)
                gain_ref[n, pl.ds(j, 1), :] = (
                    gain_in[n, pl.ds(j, 1), :] + jnp.sum(term, axis=0, keepdims=True) / gain[:, col]
                )
        for s, jj in enumerate(places):
            to = pl.ds(pl.multiple_of(UNIT * jj * k_far, UNIT), both)
            for n in range(4):
                wide_back_ref[n, to, :] = res_ref[s, n, pl.ds(res_lo, both), :]

    def full_group(step, _):
        some_heads(low + step * group, group)
        return 0

    def one_more(jj, _):
        some_heads(jj, 1)
        return 0

    groups = lax.div(high - low, group)
    lax.fori_loop(0, groups, full_group, 0)
    lax.fori_loop(low + groups * group, high, one_more, 0)
    at = 0
    for ref in back_refs:
        ref[...] = wide_back_ref[:, pl.ds(at, ref.shape[1]), :]
        at += ref.shape[1]


def assemble_kernel(heads, plan, keep_ref, got_ref, *to_refs):
    core = plan[1]
    for ref, side in ((keep_ref, core), (got_ref, 1 - core)):
        for j in range(heads):
            col = pl.multiple_of((side * heads + j) * D_HEAD, D_HEAD)
            for n in range(4):
                to_refs[n][:, pl.ds(col, D_HEAD)] = ref[n, j]


def join_kernel(heads, plan, own_ref, got_ref, to_ref):
    to_ref[:, pl.ds(pl.multiple_of(plan[1] * heads, heads), heads), :] = own_ref[...]
    to_ref[:, pl.ds(pl.multiple_of((1 - plan[1]) * heads, heads), heads), :] = got_ref[...]


def add_kernel(x_ref, y_ref, to_ref):
    to_ref[...] = x_ref[...] + y_ref[...]


def finish_kernel(rows, heads, pieces, plan, q_ref, k_ref, qg_ref, kg_ref, inv_ref, total_ref,
                  total_got_ref, *rest):
    backs, backs_got, rest = rest[:pieces], rest[pieces : 2 * pieces], rest[2 * pieces :]
    out_hbm, dq_hbm, dk_hbm, dv_hbm, qg_hbm, kg_hbm, *held = rest[4:14]
    wide_ref, dq_ref, dk_ref, sum_ref, sems = rest[14:]
    core = plan[1]
    j0, j1, k_own, row0 = own_side(plan)
    base = core * rows
    sum_ref[...] = total_ref[...] + total_got_ref[...]
    sums = [
        pltpu.make_async_copy(sum_ref.at[0], qg_hbm, sems.at[4]),
        pltpu.make_async_copy(sum_ref.at[1], kg_hbm, sems.at[5]),
    ]
    for copy in sums:
        copy.start()
    for s, refs in enumerate((backs, backs_got)):
        length = 0
        for ref in refs:
            wide_ref[s, :, pl.ds(rows + length, ref.shape[1]), :] = ref[...]
            length += ref.shape[1]
    r = lax.broadcasted_iota(jnp.int32, (rows, D_HEAD), 0) + base
    first = plan[0] == 0
    inside = (r >= jnp.where(first, plan[9] - plan[2], 0)) & (
        r < jnp.where(first, plan[9], plan[3])
    )

    def one_head(j, _):
        at = (j - j0) * k_own * UNIT + base - row0 + rows
        at = pl.multiple_of(jnp.clip(at, 0, length + rows), UNIT)
        for s, side in ((0, core), (1, 1 - core)):
            col = pl.multiple_of((side * heads + j) * D_HEAD, D_HEAD)
            for n in range(4):
                new = wide_ref[s, n, pl.ds(at, rows), :].astype(jnp.float32)
                old = held[n][:, pl.ds(col, D_HEAD)].astype(jnp.float32)
                held[n][:, pl.ds(col, D_HEAD)] = jnp.where(inside, new, old).astype(jnp.bfloat16)
        return 0

    lax.fori_loop(j0, jnp.where(k_own > 0, j1, j0), one_head, 0)
    copies = [
        pltpu.make_async_copy(held[0], out_hbm, sems.at[0]),
        pltpu.make_async_copy(held[3], dv_hbm, sems.at[1]),
        pltpu.make_async_copy(dq_ref, dq_hbm, sems.at[2]),
        pltpu.make_async_copy(dk_ref, dk_hbm, sems.at[3]),
    ]
    copies[0].start()
    copies[1].start()
    for n, (raw_ref, gain_ref, grad_ref, to_ref) in enumerate(
        ((q_ref, qg_ref, held[1], dq_ref), (k_ref, kg_ref, held[2], dk_ref))
    ):
        raw = raw_ref[...].astype(jnp.float32)
        scaled = gain_ref[...] * grad_ref[...].astype(jnp.float32)
        mean_term = jnp.mean(scaled * raw, axis=-1, keepdims=True)
        inv = inv_ref[n, :, 0:1]
        to_ref[...] = (inv * scaled - raw * (inv * inv * inv * mean_term)).astype(jnp.bfloat16)
        copies[2 + n].start()
    for copy in copies + sums:
        copy.wait()


def per_device_clips(queries, keys, values, q_gain, k_gain, out_grad, segments, visible, dp):
    rows, width = queries.shape
    heads = width // D_HEAD // CORES
    seq = segments.shape[1]
    budget = units_needed(CORES * rows // UNIT, heads)
    both = CORES * rows
    bf16, f32 = jnp.bfloat16, jnp.float32
    smem = pl.BlockSpec(memory_space=pltpu.SMEM)
    vmem = pl.BlockSpec(memory_space=pltpu.VMEM)
    hbm = pl.BlockSpec(memory_space=pl.ANY)
    limit = lambda mib: pltpu.CompilerParams(vmem_limit_bytes=mib << 20)
    keep_in_vmem = lambda x: pltpu.with_memory_space_constraint(x, pltpu.VMEM)
    swap_core = [(i, i ^ 1) for i in range(4)]
    swap_chip = [(i, i ^ 2) for i in range(4)]
    q_gain2, k_gain2 = q_gain[None], k_gain[None]
    split = pltpu.VMEM((4, heads, rows, D_HEAD), bf16)

    hbm_only = pl.BlockSpec(memory_space=pltpu.HBM)
    pair = pltpu.VMEM((2, heads, rows, D_HEAD), bf16)
    raw = pltpu.VMEM((rows, width), bf16)
    mine_vg, theirs_vg, raw_q, raw_k, plan = pl.pallas_call(
        functools.partial(fetch_kernel, heads, budget),
        in_specs=[hbm_only] * 5,
        out_specs=[vmem] * 4 + [smem],
        out_shape=[pair, pair, raw, raw, pltpu.SMEM((16,), jnp.int32)],
        scratch_shapes=[
            pltpu.VMEM((1, seq), jnp.int32),
            pltpu.SemaphoreType.DMA((3,)),
            pltpu.SemaphoreType.DMA((4 * heads,)),
        ],
        compiler_params=limit(4),
        name="fetch",
    )(*[pltpu.with_memory_space_constraint(x, pltpu.HBM)
        for x in (queries, keys, values, out_grad, segments)])
    got_vg = lax.ppermute(theirs_vg, "seq", swap_core)
    plan = pltpu.with_memory_space_constraint(plan, pltpu.SMEM)
    raw_q, raw_k, mine_vg, got_vg = (keep_in_vmem(x) for x in (raw_q, raw_k, mine_vg, got_vg))
    mine_qk, theirs_qk, inv = pl.pallas_call(
        functools.partial(prepare_kernel, rows, heads),
        in_specs=[smem] + [vmem] * 4,
        out_specs=[vmem] * 3,
        out_shape=[pair, pair, pltpu.VMEM((2, rows, D_HEAD), f32)],
        compiler_params=limit(8),
        name="prepare",
    )(plan, raw_q, raw_k, q_gain2, k_gain2)
    got_qk = lax.ppermute(theirs_qk, "seq", swap_core)
    mine_qk, got_qk = keep_in_vmem(mine_qk), keep_in_vmem(got_qk)

    ends = [0, *(budget * n // 4 for n in PARTS), budget]
    sizes = [y - x for x, y in zip(ends, ends[1:])]

    def pack(units, mine, got):
        return pl.pallas_call(
            functools.partial(pack_kernel, rows),
            in_specs=[smem, vmem, vmem],
            out_specs=[vmem] * len(units),
            out_shape=[pltpu.VMEM((2, n * UNIT, D_HEAD), bf16) for n in units],
            compiler_params=limit(4),
        )(plan, mine, got)

    send_vg = pack([budget], mine_vg, got_vg)[0]
    far_vg = keep_in_vmem(lax.ppermute(send_vg, "seq", swap_chip))
    fars = []
    for x in pack(sizes, mine_qk, got_qk):
        fars.append(keep_in_vmem(lax.ppermute(x, "seq", swap_chip)))

    gains_shape = pltpu.VMEM((2, heads, D_HEAD), f32)
    keep, give, gain_part, cross_bias, place = pl.pallas_call(
        functools.partial(local_kernel, rows, heads, LOCAL_GROUP),
        in_specs=[smem] + [vmem] * 8,
        out_specs=[vmem] * 5,
        out_shape=[
            split,
            split,
            gains_shape,
            pltpu.VMEM((both, both), f32),
            pltpu.VMEM((2, both, D_HEAD), bf16),
        ],
        scratch_shapes=[pltpu.VMEM((both, both), f32), pltpu.VMEM((both, D_HEAD), f32)],
        compiler_params=limit(16),
        name="local",
    )(plan, mine_qk, mine_vg, got_qk, got_vg, segments, visible, q_gain2, k_gain2)

    length = budget * UNIT
    wide_back = None
    for stage in range(len(sizes)):
        last = stage == len(sizes) - 1
        args = [plan, mine_qk, mine_vg, got_qk, got_vg, far_vg, *fars[: stage + 1]]
        args += [keep_in_vmem(cross_bias), keep_in_vmem(place), q_gain2, k_gain2]
        args += [keep_in_vmem(x) for x in (gain_part, keep, give)]
        aliases = {len(args) - 2: 0, len(args) - 1: 1}
        if stage:
            aliases[len(args)] = 3
            args.append(keep_in_vmem(wide_back))

        def body(*refs, stage=stage, count=len(args), last=last):
            ins, outs = refs[:count], list(refs[count:])
            outs[4 : 4 + last] = [outs[4 : 4 + last]]
            at = 7 + stage
            crossing_kernel(rows, heads, stage, len(sizes), CROSS_GROUP, ins[0], ins[1:3],
                            ins[3:5], ins[5], ins[6:at], *ins[at : at + 5], *outs)

        keep, give, gain_part, wide_back, *backs = pl.pallas_call(
            body,
            in_specs=[smem] + [vmem] * (len(args) - 1),
            out_specs=[vmem] * (4 + last),
            out_shape=[split, split, gains_shape, pltpu.VMEM((4, length + both, D_HEAD), bf16)]
            + [pltpu.VMEM((4, length, D_HEAD), bf16)] * last,
            input_output_aliases=aliases,
            scratch_shapes=[
                pltpu.VMEM((4, length + 2 * both, D_HEAD), bf16),
                pltpu.VMEM((CROSS_GROUP, 4, 2 * both, D_HEAD), bf16),
            ],
            compiler_params=limit(20),
        )(*args)

    gain_far = lax.ppermute(gain_part, "seq", swap_chip)
    backs = [lax.ppermute(x, "seq", swap_chip) for x in backs]
    res_got = keep_in_vmem(lax.ppermute(give, "seq", swap_core))
    add = lambda x, y: pl.pallas_call(
        add_kernel,
        in_specs=[vmem, vmem],
        out_specs=vmem,
        out_shape=pltpu.VMEM(x.shape, f32),
        compiler_params=limit(1),
        name="add",
    )(keep_in_vmem(x), keep_in_vmem(y))
    gain_part = add(gain_part, gain_far)
    gain_got = lax.ppermute(gain_part, "seq", swap_core)
    total = pl.pallas_call(
        functools.partial(join_kernel, heads),
        in_specs=[smem, vmem, vmem],
        out_specs=vmem,
        out_shape=pltpu.VMEM((2, CORES * heads, D_HEAD), f32),
        compiler_params=limit(1),
        name="join",
    )(plan, keep_in_vmem(gain_part), keep_in_vmem(gain_got))
    step = 1
    while step < dp:
        total_got = lax.ppermute(total, "dp", [(i, i ^ step) for i in range(dp)])
        step = 2 * step
        if step < dp:
            total = add(total, total_got)

    held = pl.pallas_call(
        functools.partial(assemble_kernel, heads),
        in_specs=[smem, vmem, vmem],
        out_specs=[vmem] * 4,
        out_shape=[pltpu.VMEM((rows, width), bf16)] * 4,
        compiler_params=limit(4),
        name="assemble",
    )(plan, keep_in_vmem(keep), res_got)

    backs[-1], total, held = lax.optimization_barrier((backs[-1], total, held))
    backs_got = []
    for x in backs:
        backs_got.append(keep_in_vmem(lax.ppermute(x, "seq", swap_core)))
    backs = [keep_in_vmem(x) for x in backs]

    full = jax.ShapeDtypeStruct((rows, width), bf16)
    args = [plan, raw_q, raw_k, q_gain2, k_gain2, keep_in_vmem(inv)]
    args += [keep_in_vmem(total), keep_in_vmem(total_got), *backs, *backs_got]
    args += [keep_in_vmem(x) for x in held]
    outs = pl.pallas_call(
        functools.partial(finish_kernel, rows, heads, len(backs)),
        in_specs=[smem] + [vmem] * (len(args) - 1),
        out_specs=[hbm] * 6 + [vmem] * 4,
        out_shape=[full] * 4
        + [jax.ShapeDtypeStruct((CORES * heads, D_HEAD), f32)] * 2
        + [pltpu.VMEM((rows, width), bf16)] * 4,
        input_output_aliases={len(args) - 4 + i: 6 + i for i in range(4)},
        scratch_shapes=[
            pltpu.VMEM((2, 4, length + 2 * rows, D_HEAD), bf16),
            pltpu.VMEM((rows, width), bf16),
            pltpu.VMEM((rows, width), bf16),
            pltpu.VMEM((2, CORES * heads, D_HEAD), f32),
            pltpu.SemaphoreType.DMA((6,)),
        ],
        compiler_params=limit(12),
        name="finish",
    )(*args)
    attn_out, query_grad, key_grad, value_grad = outs[:4]
    return (attn_out, query_grad, key_grad, value_grad, *(x.reshape(width) for x in outs[4:6]))


def solution(mesh):
    dp, seq = mesh.shape["dp"], mesh.shape["seq"]
    two_chips = seq == 2 * CORES and dp > 1 and dp & (dp - 1) == 0

    def per_device(queries, keys, values, q_gain, k_gain, out_grad, segments, visible):
        args = (queries, keys, values, q_gain, k_gain, out_grad, segments, visible)
        if two_chips:
            return per_device_clips(*args, dp)
        return per_device_any(*args)

    rows = P(("dp", "seq"), None)
    return jax.shard_map(
        per_device,
        mesh=mesh,
        in_specs=(rows, rows, rows, P(), P(), rows, P("dp", None), P("dp", None)),
        out_specs=(rows, rows, rows, rows, P(), P()),
        check_vma=False,
    )
```

```python
import functools

import jax
import jax.numpy as jnp
from jax import lax
from jax.experimental import pallas as pl
from jax.experimental.pallas import tpu as pltpu
from jax.sharding import PartitionSpec as P


D_HEAD = 128
UNIT = 16
CORES = 2
EPSILON = 1e-06
NEG = -1e30
LOCAL_GROUP = 4
CROSS_GROUP = 2
PARTS = (2, 3)


def normalize(raw_rows, gain_vec):
    raw_f32 = raw_rows.astype(jnp.float32)
    inv_rms = lax.rsqrt(jnp.mean(raw_f32 * raw_f32, axis=-1, keepdims=True) + EPSILON)
    return ((raw_f32 * inv_rms * gain_vec).astype(jnp.bfloat16), inv_rms)


def norm_back(raw_rows, inv_rms, gain_vec, grad_norm):
    raw_f32 = raw_rows.astype(jnp.float32)
    grad_f32 = grad_norm.astype(jnp.float32)
    scaled_grad = gain_vec * grad_f32
    mean_term = jnp.mean(scaled_grad * raw_f32, axis=-1, keepdims=True)
    grad_raw = inv_rms * scaled_grad - raw_f32 * inv_rms**3 * mean_term
    return (grad_raw.astype(jnp.bfloat16), jnp.sum(grad_f32 * raw_f32 * inv_rms, axis=0))


def attend(q_norm, k_norm, val_rows, grad_rows, seg_row, vis_row):
    seq_rows, feature_count = q_norm.shape
    heads = feature_count // D_HEAD
    scale = D_HEAD ** (-0.5)
    positions = jnp.arange(seq_rows, dtype=jnp.int32)
    allowed = (seg_row[:, None] == seg_row[None, :]) & (
        (vis_row[None, :] == 1) | (positions[:, None] == positions[None, :])
    )
    f32 = jnp.float32
    q, k, v, g = (
        x.reshape(seq_rows, heads, D_HEAD) for x in (q_norm, k_norm, val_rows, grad_rows)
    )
    scores = jnp.einsum("shd,thd->hst", q, k, preferred_element_type=f32) * scale
    scores = jnp.where(allowed[None], scores, NEG)
    weights = jnp.exp(scores - jnp.max(scores, axis=-1, keepdims=True))
    prob = weights / jnp.sum(weights, axis=-1, keepdims=True)
    half = prob.astype(jnp.bfloat16)
    out = jnp.einsum("hst,thd->shd", half, v, preferred_element_type=f32)
    dprob = jnp.einsum("shd,thd->hst", g, v, preferred_element_type=f32)
    v_grad = jnp.einsum("hst,shd->thd", half, g, preferred_element_type=f32)
    row_dot = jnp.sum(prob * dprob, axis=-1, keepdims=True)
    score_grad = (prob * (dprob - row_dot) * scale).astype(jnp.bfloat16)
    q_grad = jnp.einsum("hst,thd->shd", score_grad, k, preferred_element_type=f32)
    k_grad = jnp.einsum("hst,shd->thd", score_grad, q, preferred_element_type=f32)
    return tuple(
        x.reshape(seq_rows, feature_count).astype(jnp.bfloat16)
        for x in (out, q_grad, k_grad, v_grad)
    )


def per_device_any(queries, keys, values, q_gain, k_gain, out_grad, segments, visible):
    q_norm, q_inv = normalize(queries, q_gain)
    k_norm, k_inv = normalize(keys, k_gain)
    gather = functools.partial(
        lax.all_to_all, axis_name="seq", split_axis=1, concat_axis=0, tiled=True
    )
    spread = functools.partial(
        lax.all_to_all, axis_name="seq", split_axis=0, concat_axis=1, tiled=True
    )
    parts = attend(
        *(gather(x) for x in (q_norm, k_norm, values, out_grad)), segments[0], visible[0]
    )
    attn_out, q_grad, k_grad, value_grad = (spread(x) for x in parts)
    query_grad, q_gain_part = norm_back(queries, q_inv, q_gain, q_grad)
    key_grad, k_gain_part = norm_back(keys, k_inv, k_gain, k_grad)
    q_gain_grad, k_gain_grad = lax.psum((q_gain_part, k_gain_part), ("dp", "seq"))
    return (attn_out, query_grad, key_grad, value_grad, q_gain_grad, k_gain_grad)


def units_needed(blocks, heads):
    worst = 0
    for ka in range(1, blocks + 1):
        for kb in range(1, blocks + 2 - ka):
            worst = max(worst, min(max(ka * (heads - h), kb * h) for h in range(heads + 1)))
    return worst


def dot(x, y, dims):
    return lax.dot_general(x, y, (dims, ((), ())), preferred_element_type=jnp.float32)


NT = ((1,), (1,))
NN = ((1,), (0,))
TN = ((0,), (0,))
LOG2_E = 1.4426950408889634


def attention(q, k, v, g, bias):
    scale = D_HEAD ** (-0.5)
    scores = dot(k, q, NT) * (scale * LOG2_E) + bias
    weights = jnp.exp2(scores - jnp.max(scores, axis=0, keepdims=True))
    prob = weights * (1.0 / jnp.sum(weights, axis=0, keepdims=True))
    half = prob.astype(jnp.bfloat16)
    out = dot(half, v, TN)
    dprob = dot(v, g, NT)
    v_grad = dot(half, g, NN)
    row_dot = jnp.sum(prob * dprob, axis=0, keepdims=True)
    score_grad = (prob * scale * (dprob - row_dot)).astype(jnp.bfloat16)
    q_grad = dot(score_grad, k, TN)
    k_grad = dot(score_grad, q, NN)
    return tuple(x.astype(jnp.bfloat16) for x in (out, q_grad, k_grad, v_grad))


def own_side(plan):
    first = plan[0] == 0
    heads = plan[8]
    j0 = jnp.where(first, plan[6], 0)
    j1 = jnp.where(first, heads, plan[6])
    k_own = jnp.where(first, plan[4], plan[5])
    row0 = jnp.where(first, plan[9] - UNIT * plan[4], 0)
    return j0, j1, k_own, row0


def fetch_kernel(heads, v_hbm, g_hbm, qg_hbm, kg_hbm, seg_hbm, mine_ref, theirs_ref, qg_ref, kg_ref,
                 seg_ref, sems, head_sems):
    core = lax.rem(lax.axis_index("seq"), CORES)
    copies = []

    def fetch(source, target, sem):
        copy = pltpu.make_async_copy(source, target, sem)
        copy.start()
        copies.append(copy)

    for half, target in ((1 - core, theirs_ref), (core, mine_ref)):
        for n, source in enumerate((v_hbm, g_hbm)):
            for j in range(heads):
                col = pl.ds(pl.multiple_of((half * heads + j) * D_HEAD, D_HEAD), D_HEAD)
                fetch(source.at[:, col], target.at[n, j], head_sems.at[len(copies)])
    for n, pair in enumerate(((qg_hbm, qg_ref), (kg_hbm, kg_ref), (seg_hbm, seg_ref))):
        fetch(*pair, sems.at[n])
    for copy in copies:
        copy.wait()


def prepare_kernel(rows, heads, budget, q_ref, k_ref, qg_ref, kg_ref, seg_ref, mine_ref, theirs_ref,
                   inv_ref, plan_ref):
    core = lax.rem(lax.axis_index("seq"), CORES)
    seg = seg_ref[...].astype(jnp.float32)
    chip_rows = seg.shape[1] // 2
    at = lax.broadcasted_iota(jnp.int32, seg.shape, 1)
    edge = jnp.sum(jnp.where(at == chip_rows - 1, seg, 0.0))
    beyond = jnp.sum(jnp.where(at == chip_rows, seg, 0.0))
    crosses = edge == beyond
    same = seg == edge
    a = jnp.sum(jnp.where(same & (at < chip_rows), 1.0, 0.0)).astype(jnp.int32)
    b = jnp.sum(jnp.where(same & (at >= chip_rows), 1.0, 0.0)).astype(jnp.int32)
    a = jnp.where(crosses, a, 0)
    b = jnp.where(crosses, b, 0)
    ka = lax.div(a + UNIT - 1, UNIT)
    kb = lax.div(b + UNIT - 1, UNIT)
    least = jnp.int32(0)
    most = jnp.int32(0)
    for h in range(heads):
        least += (ka * (heads - h) > budget).astype(jnp.int32)
        most += (kb * (h + 1) <= budget).astype(jnp.int32)
    plan_ref[0] = lax.div(lax.axis_index("seq"), CORES)
    plan_ref[1] = core
    plan_ref[2] = a
    plan_ref[3] = b
    plan_ref[4] = ka
    plan_ref[5] = kb
    plan_ref[6] = jnp.minimum(jnp.maximum(heads // 2, least), most)
    plan_ref[7] = crosses.astype(jnp.int32)
    plan_ref[8] = jnp.int32(heads)
    plan_ref[9] = jnp.int32(chip_rows)

    for n, (raw_ref, gain_ref) in enumerate(((q_ref, qg_ref), (k_ref, kg_ref))):
        raw = raw_ref[...].astype(jnp.float32)
        inv = lax.rsqrt(jnp.mean(raw * raw, axis=-1, keepdims=True) + EPSILON)
        inv_ref[n] = jnp.broadcast_to(inv, (rows, D_HEAD))
        normed = (raw * inv * gain_ref[...]).astype(jnp.bfloat16)
        pieces = [normed[:, j * D_HEAD : (j + 1) * D_HEAD] for j in range(2 * heads)]

        @pl.when(core == 0)
        def _():
            for j in range(heads):
                mine_ref[n, j] = pieces[j]
                theirs_ref[n, j] = pieces[heads + j]

        @pl.when(core == 1)
        def _():
            for j in range(heads):
                mine_ref[n, j] = pieces[heads + j]
                theirs_ref[n, j] = pieces[j]


def pack_kernel(rows, plan, mine_ref, got_ref, *send_refs):
    core = plan[1]
    j0, j1, k_own, row0 = own_side(plan)
    for ref, half in ((mine_ref, core), (got_ref, 1 - core)):
        base = half * rows
        low = jnp.clip(lax.div(base - row0, UNIT), 0, k_own)
        high = jnp.clip(lax.div(base + rows - row0, UNIT), 0, k_own)

        def one_head(j, _, ref=ref, base=base, low=low, high=high):
            start = (j - j0) * k_own

            def unit_into(send_ref, shift):
                def one_unit(i, _):
                    at = pl.multiple_of(row0 + UNIT * i - base, UNIT)
                    to = pl.multiple_of((start + i - shift) * UNIT, UNIT)
                    for n in range(2):
                        send_ref[n, pl.ds(to, UNIT), :] = ref[n, j, pl.ds(at, UNIT), :]
                    return 0

                return one_unit

            shift, done = 0, low
            for n, send_ref in enumerate(send_refs):
                units = send_ref.shape[1] // UNIT
                last = n == len(send_refs) - 1
                cut = high if last else jnp.clip(shift + units - start, low, high)
                lax.fori_loop(done, cut, unit_into(send_ref, shift), 0)
                shift, done = shift + units, cut
            return 0

        lax.fori_loop(j0, j1, one_head, 0)


def local_kernel(rows, heads, group, plan, mine_qk, mine_vg, got_qk, got_vg, seg_ref, vis_ref, qg_ref, kg_ref,
                 keep_ref, give_ref, gain_ref, cross_bias_ref, place_ref, bias_ref, ok_ref):
    both = 2 * rows
    core, first = plan[1], plan[0] * both
    mine = [mine_qk.at[0], mine_qk.at[1], mine_vg.at[0], mine_vg.at[1]]
    got = [got_qk.at[0], got_qk.at[1], got_vg.at[0], got_vg.at[1]]

    def chip_row(ref):
        wide = ref[...].astype(jnp.float32)
        total = wide.shape[1]
        wide = jnp.broadcast_to(wide, (8, total))
        own = pltpu.roll(wide, lax.rem(2 * total - first - core * rows, total), 1)
        other = pltpu.roll(wide, lax.rem(2 * total - first - (1 - core) * rows, total), 1)
        return jnp.concatenate([own[:, :rows], other[:, :rows]], axis=1)[0:1]

    seg = jnp.broadcast_to(chip_row(seg_ref), (both, both))
    code = jnp.broadcast_to(chip_row(seg_ref) * 2.0 + chip_row(vis_ref), (both, both))
    code_t = jnp.transpose(code)
    i = lax.broadcasted_iota(jnp.int32, (both, both), 0)
    j = lax.broadcasted_iota(jnp.int32, (both, both), 1)
    gap = code_t - 2.0 * seg
    allowed = (gap == 1.0) | (i == j)
    bias_ref[...] = jnp.where(allowed, 0.0, NEG)
    r = lax.broadcasted_iota(jnp.int32, (both, D_HEAD), 0)
    at = jnp.where(r < rows, core * rows + r, (1 - core) * rows + r - rows) + first
    edge = plan[9]
    crossing = (at >= edge - plan[2]) & (at < edge + plan[3])
    ok_ref[...] = jnp.where(crossing, 0.0, 1.0)
    wide = jnp.broadcast_to(vis_ref[...].astype(jnp.float32), (8, 2 * both))
    in_first, in_last = j >= both - plan[2], j < plan[3]
    vis = jnp.where(in_first[:8], wide[:, :both], wide[:, both:])
    vis = jnp.broadcast_to(vis[0:1], (both, both)) > 0.5
    in_clip = (in_first | in_last) & ((i >= both - plan[2]) | (i < plan[3]))
    allowed = jnp.transpose(jnp.where(in_clip & vis, 1.0, 0.0)) > 0.5
    cross_bias_ref[...] = jnp.where(allowed | (i == j), 0.0, NEG)
    low, high = r < plan[3], r >= both - plan[2]
    is_first = (r >= 0) & (plan[0] == 0)
    from_own = jnp.where(is_first, jnp.where(high, 1.0, 0.0), jnp.where(low, 1.0, 0.0))
    from_far = jnp.where(is_first, jnp.where(low, 1.0, 0.0), jnp.where(high, 1.0, 0.0))
    place_ref[0] = from_own.astype(jnp.bfloat16)
    place_ref[1] = from_far.astype(jnp.bfloat16)

    def some_heads(step, _):
        for h in range(group):
            j = step * group + h
            q, k, v, g = (
                jnp.concatenate([mine[n][j], got[n][j]], axis=0) for n in range(4)
            )
            results = attention(q, k, v, g, bias_ref[...])
            for n, x in enumerate(results):
                keep_ref[n, j] = x[:rows]
                give_ref[n, j] = x[rows:]
            col = pl.ds(pl.multiple_of((core * heads + j) * D_HEAD, D_HEAD), D_HEAD)
            ok = ok_ref[...]
            for n, (x, y, gain) in enumerate(
                ((q, results[1], qg_ref), (k, results[2], kg_ref))
            ):
                term = ok * x.astype(jnp.float32) * y.astype(jnp.float32)
                gain_ref[n, pl.ds(j, 1), :] = jnp.sum(term, axis=0, keepdims=True) / gain[:, col]
        return 0

    lax.fori_loop(0, heads // group, some_heads, 0)


def crossing_kernel(rows, heads, stage, stages, group, plan, mine_refs, got_refs, far_vg, far_refs, bias_ref,
                    place_ref, qg_ref, kg_ref, gain_in, keep_ref, give_ref, gain_ref, wide_back_ref,
                    back_refs, far_ref, res_ref):
    both = 2 * rows
    core, first = plan[1], plan[0] == 0
    k_far = jnp.where(first, plan[5], plan[4])
    j0 = jnp.where(first, 0, plan[6])
    count = jnp.where(plan[7] == 1, jnp.where(first, plan[6], heads - plan[6]), 0)
    units = [ref.shape[1] // UNIT for ref in far_refs]
    ready = lambda n: jnp.minimum(lax.div(n, jnp.maximum(k_far, 1)), count)
    low = ready(sum(units[:-1])) if stage else 0
    high = ready(sum(units)) if stage < stages - 1 else count

    @pl.when(high > low)
    def _():
        at = both
        for ref in far_refs:
            far_ref[0:2, pl.ds(at, ref.shape[1]), :] = ref[...]
            at += ref.shape[1]
        far_ref[2:4, pl.ds(both, far_vg.shape[1]), :] = far_vg[...]

    gain_ref[...] = gain_in[...]
    far_lo = jnp.where(first, both, UNIT * k_far)
    res_lo = pl.multiple_of(jnp.where(first, 0, both - UNIT * k_far), UNIT)

    def some_heads(jj_first, group):
        places = [jj_first + s for s in range(group)]
        from_own, from_far = place_ref[0] > 0.5, place_ref[1] > 0.5
        for s, jj in enumerate(places):
            j = j0 + jj
            far = pl.ds(pl.multiple_of(far_lo + UNIT * jj * k_far, UNIT), both)
            loaded = []
            for n in range(4):
                mine, got = mine_refs[n // 2][n % 2, j], got_refs[n // 2][n % 2, j]
                own = jnp.where(
                    core == 0,
                    jnp.concatenate([mine, got], axis=0),
                    jnp.concatenate([got, mine], axis=0),
                )
                distant = jnp.where(from_far, far_ref[n, far, :], jnp.zeros_like(own))
                loaded.append(jnp.where(from_own, own, distant))
            q, k, v, g = loaded
            results = attention(q, k, v, g, bias_ref[...])
            own_rows = pl.ds(pl.multiple_of(core * rows, rows), rows)
            got_rows = pl.ds(pl.multiple_of((1 - core) * rows, rows), rows)
            for n, x in enumerate(results):
                res_ref[s, n, pl.ds(0, both), :] = x
            for here, ref in ((own_rows, keep_ref), (got_rows, give_ref)):
                ours = place_ref[0, here, :] > 0.5
                for n in range(4):
                    ref[n, j] = jnp.where(ours, res_ref[s, n, here, :], ref[n, j])
            col = pl.ds(pl.multiple_of((core * heads + j) * D_HEAD, D_HEAD), D_HEAD)
            for n, (x, y, gain) in enumerate(
                ((q, results[1], qg_ref), (k, results[2], kg_ref))
            ):
                term = x.astype(jnp.float32) * y.astype(jnp.float32)
                gain_ref[n, pl.ds(j, 1), :] = (
                    gain_in[n, pl.ds(j, 1), :] + jnp.sum(term, axis=0, keepdims=True) / gain[:, col]
                )
        for s, jj in enumerate(places):
            to = pl.ds(pl.multiple_of(UNIT * jj * k_far, UNIT), both)
            for n in range(4):
                wide_back_ref[n, to, :] = res_ref[s, n, pl.ds(res_lo, both), :]

    def full_group(step, _):
        some_heads(low + step * group, group)
        return 0

    def one_more(jj, _):
        some_heads(jj, 1)
        return 0

    groups = lax.div(high - low, group)
    lax.fori_loop(0, groups, full_group, 0)
    lax.fori_loop(low + groups * group, high, one_more, 0)
    at = 0
    for ref in back_refs:
        ref[...] = wide_back_ref[:, pl.ds(at, ref.shape[1]), :]
        at += ref.shape[1]


def assemble_kernel(heads, plan, keep_ref, got_ref, *to_refs):
    core = plan[1]
    for ref, side in ((keep_ref, core), (got_ref, 1 - core)):
        for j in range(heads):
            col = pl.multiple_of((side * heads + j) * D_HEAD, D_HEAD)
            for n in range(4):
                to_refs[n][:, pl.ds(col, D_HEAD)] = ref[n, j]


def join_kernel(heads, plan, own_ref, got_ref, to_ref):
    to_ref[:, pl.ds(pl.multiple_of(plan[1] * heads, heads), heads), :] = own_ref[...]
    to_ref[:, pl.ds(pl.multiple_of((1 - plan[1]) * heads, heads), heads), :] = got_ref[...]


def add_kernel(x_ref, y_ref, to_ref):
    to_ref[...] = x_ref[...] + y_ref[...]


def overlay(rows, heads, plan, side, back_ref, wide_ref, held):
    j0, j1, k_own, row0 = own_side(plan)
    base = plan[1] * rows
    length = back_ref.shape[1]
    wide_ref[:, pl.ds(rows, length), :] = back_ref[...]
    r = lax.broadcasted_iota(jnp.int32, (rows, D_HEAD), 0) + base
    first = plan[0] == 0
    inside = (r >= jnp.where(first, plan[9] - plan[2], 0)) & (
        r < jnp.where(first, plan[9], plan[3])
    )
    inside = jnp.where(inside, 1.0, 0.0).astype(jnp.bfloat16)

    def one_head(j, _):
        at = (j - j0) * k_own * UNIT + base - row0 + rows
        at = pl.multiple_of(jnp.clip(at, 0, length + rows), UNIT)
        col = pl.multiple_of((side * heads + j) * D_HEAD, D_HEAD)
        for n in range(4):
            new = wide_ref[n, pl.ds(at, rows), :]
            old = held[n][:, pl.ds(col, D_HEAD)]
            held[n][:, pl.ds(col, D_HEAD)] = jnp.where(inside > 0.5, new, old)
        return 0

    lax.fori_loop(j0, jnp.where(k_own > 0, j1, j0), one_head, 0)


def overlay_kernel(rows, heads, plan, back_ref, *rest):
    overlay(rows, heads, plan, plan[1], back_ref, rest[8], rest[4:8])


def finish_kernel(rows, heads, plan, q_ref, k_ref, qg_ref, kg_ref, inv_ref, total_ref,
                  total_got_ref, back_got_ref, *rest):
    out_hbm, dq_hbm, dk_hbm, dv_hbm, qg_hbm, kg_hbm, *held = rest[4:14]
    wide_ref, dq_ref, dk_ref, sum_ref, sems = rest[14:]
    overlay(rows, heads, plan, 1 - plan[1], back_got_ref, wide_ref, held)
    sum_ref[...] = total_ref[...] + total_got_ref[...]
    copies = [
        pltpu.make_async_copy(held[0], out_hbm, sems.at[0]),
        pltpu.make_async_copy(held[3], dv_hbm, sems.at[1]),
        pltpu.make_async_copy(sum_ref.at[0], qg_hbm, sems.at[2]),
        pltpu.make_async_copy(sum_ref.at[1], kg_hbm, sems.at[3]),
    ]
    for copy in copies:
        copy.start()
    half = rows // 2
    for n, (raw_ref, gain_ref, grad_ref, to_ref, to_hbm) in enumerate(
        ((q_ref, qg_ref, held[1], dq_ref, dq_hbm), (k_ref, kg_ref, held[2], dk_ref, dk_hbm))
    ):
        for part in range(2):
            here = pl.ds(part * half, half)
            raw = raw_ref[here, :].astype(jnp.float32)
            scaled = gain_ref[...] * grad_ref[here, :].astype(jnp.float32)
            mean_term = jnp.mean(scaled * raw, axis=-1, keepdims=True)
            inv = inv_ref[n, here, 0:1]
            grad = inv * scaled - raw * (inv * inv * inv * mean_term)
            to_ref[here, :] = grad.astype(jnp.bfloat16)
            copy = pltpu.make_async_copy(
                to_ref.at[here], to_hbm.at[here], sems.at[4 + 2 * n + part]
            )
            copy.start()
            copies.append(copy)
    for copy in copies:
        copy.wait()


def per_device_clips(queries, keys, values, q_gain, k_gain, out_grad, segments, visible, dp):
    rows, width = queries.shape
    heads = width // D_HEAD // CORES
    seq = segments.shape[1]
    budget = units_needed(CORES * rows // UNIT, heads)
    both = CORES * rows
    bf16, f32 = jnp.bfloat16, jnp.float32
    smem = pl.BlockSpec(memory_space=pltpu.SMEM)
    vmem = pl.BlockSpec(memory_space=pltpu.VMEM)
    hbm = pl.BlockSpec(memory_space=pl.ANY)
    limit = lambda mib: pltpu.CompilerParams(vmem_limit_bytes=mib << 20)
    keep_in_vmem = lambda x: pltpu.with_memory_space_constraint(x, pltpu.VMEM)
    swap_core = [(i, i ^ 1) for i in range(4)]
    swap_chip = [(i, i ^ 2) for i in range(4)]
    split = pltpu.VMEM((4, heads, rows, D_HEAD), bf16)

    hbm_only = pl.BlockSpec(memory_space=pltpu.HBM)
    pair = pltpu.VMEM((2, heads, rows, D_HEAD), bf16)
    mine_vg, theirs_vg, q_gain2, k_gain2, seg_row = pl.pallas_call(
        functools.partial(fetch_kernel, heads),
        in_specs=[hbm_only] * 5,
        out_specs=[vmem] * 5,
        out_shape=[
            pair,
            pair,
            pltpu.VMEM((1, width), f32),
            pltpu.VMEM((1, width), f32),
            pltpu.VMEM((1, seq), jnp.int32),
        ],
        scratch_shapes=[
            pltpu.SemaphoreType.DMA((3,)),
            pltpu.SemaphoreType.DMA((4 * heads,)),
        ],
        compiler_params=limit(4),
        name="fetch",
    )(*[pltpu.with_memory_space_constraint(x, pltpu.HBM)
        for x in (values, out_grad, q_gain[None], k_gain[None], segments)])
    got_vg = lax.ppermute(theirs_vg, "seq", swap_core)
    raw_q, raw_k, mine_vg, got_vg = (keep_in_vmem(x) for x in (queries, keys, mine_vg, got_vg))
    q_gain2, k_gain2, seg_row = (keep_in_vmem(x) for x in (q_gain2, k_gain2, seg_row))
    mine_qk, theirs_qk, inv, plan = pl.pallas_call(
        functools.partial(prepare_kernel, rows, heads, budget),
        in_specs=[vmem] * 5,
        out_specs=[vmem] * 3 + [smem],
        out_shape=[
            pair,
            pair,
            pltpu.VMEM((2, rows, D_HEAD), f32),
            pltpu.SMEM((16,), jnp.int32),
        ],
        compiler_params=limit(8),
        name="prepare",
    )(raw_q, raw_k, q_gain2, k_gain2, seg_row)
    plan = pltpu.with_memory_space_constraint(plan, pltpu.SMEM)
    got_qk = lax.ppermute(theirs_qk, "seq", swap_core)
    mine_qk, got_qk = keep_in_vmem(mine_qk), keep_in_vmem(got_qk)

    ends = [0, *(budget * n // 4 for n in PARTS), budget]
    sizes = [y - x for x, y in zip(ends, ends[1:])]

    def pack(units, mine, got):
        return pl.pallas_call(
            functools.partial(pack_kernel, rows),
            in_specs=[smem, vmem, vmem],
            out_specs=[vmem] * len(units),
            out_shape=[pltpu.VMEM((2, n * UNIT, D_HEAD), bf16) for n in units],
            compiler_params=limit(4),
        )(plan, mine, got)

    send_vg = pack([budget], mine_vg, got_vg)[0]
    far_vg = keep_in_vmem(lax.ppermute(send_vg, "seq", swap_chip))
    fars = []
    for x in pack(sizes, mine_qk, got_qk):
        fars.append(keep_in_vmem(lax.ppermute(x, "seq", swap_chip)))

    gains_shape = pltpu.VMEM((2, heads, D_HEAD), f32)
    keep, give, gain_part, cross_bias, place = pl.pallas_call(
        functools.partial(local_kernel, rows, heads, LOCAL_GROUP),
        in_specs=[smem] + [vmem] * 8,
        out_specs=[vmem] * 5,
        out_shape=[
            split,
            split,
            gains_shape,
            pltpu.VMEM((both, both), f32),
            pltpu.VMEM((2, both, D_HEAD), bf16),
        ],
        scratch_shapes=[pltpu.VMEM((both, both), f32), pltpu.VMEM((both, D_HEAD), f32)],
        compiler_params=limit(16),
        name="local",
    )(plan, mine_qk, mine_vg, got_qk, got_vg, seg_row, visible, q_gain2, k_gain2)

    length = budget * UNIT
    wide_back = None
    for stage in range(len(sizes)):
        last = stage == len(sizes) - 1
        args = [plan, mine_qk, mine_vg, got_qk, got_vg, far_vg, *fars[: stage + 1]]
        args += [keep_in_vmem(cross_bias), keep_in_vmem(place), q_gain2, k_gain2]
        args += [keep_in_vmem(x) for x in (gain_part, keep, give)]
        aliases = {len(args) - 2: 0, len(args) - 1: 1}
        if stage:
            aliases[len(args)] = 3
            args.append(keep_in_vmem(wide_back))

        def body(*refs, stage=stage, count=len(args), last=last):
            ins, outs = refs[:count], list(refs[count:])
            outs[4 : 4 + last] = [outs[4 : 4 + last]]
            at = 7 + stage
            crossing_kernel(rows, heads, stage, len(sizes), CROSS_GROUP, ins[0], ins[1:3],
                            ins[3:5], ins[5], ins[6:at], *ins[at : at + 5], *outs)

        keep, give, gain_part, wide_back, *backs = pl.pallas_call(
            body,
            in_specs=[smem] + [vmem] * (len(args) - 1),
            out_specs=[vmem] * (4 + last),
            out_shape=[split, split, gains_shape, pltpu.VMEM((4, length + both, D_HEAD), bf16)]
            + [pltpu.VMEM((4, length, D_HEAD), bf16)] * last,
            input_output_aliases=aliases,
            scratch_shapes=[
                pltpu.VMEM((4, length + 2 * both, D_HEAD), bf16),
                pltpu.VMEM((CROSS_GROUP, 4, 2 * both, D_HEAD), bf16),
            ],
            compiler_params=limit(20),
        )(*args)

    gain_far = lax.ppermute(gain_part, "seq", swap_chip)
    backs = [lax.ppermute(x, "seq", swap_chip) for x in backs]
    res_got = keep_in_vmem(lax.ppermute(give, "seq", swap_core))
    add = lambda x, y: pl.pallas_call(
        add_kernel,
        in_specs=[vmem, vmem],
        out_specs=vmem,
        out_shape=pltpu.VMEM(x.shape, f32),
        compiler_params=limit(1),
        name="add",
    )(keep_in_vmem(x), keep_in_vmem(y))
    gain_part = add(gain_part, gain_far)
    gain_got = lax.ppermute(gain_part, "seq", swap_core)
    total = pl.pallas_call(
        functools.partial(join_kernel, heads),
        in_specs=[smem, vmem, vmem],
        out_specs=vmem,
        out_shape=pltpu.VMEM((2, CORES * heads, D_HEAD), f32),
        compiler_params=limit(1),
        name="join",
    )(plan, keep_in_vmem(gain_part), keep_in_vmem(gain_got))
    step = 1
    while step < dp:
        total_got = lax.ppermute(total, "dp", [(i, i ^ step) for i in range(dp)])
        step = 2 * step
        if step < dp:
            total = add(total, total_got)

    held = pl.pallas_call(
        functools.partial(assemble_kernel, heads),
        in_specs=[smem, vmem, vmem],
        out_specs=[vmem] * 4,
        out_shape=[pltpu.VMEM((rows, width), bf16)] * 4,
        compiler_params=limit(4),
        name="assemble",
    )(plan, keep_in_vmem(keep), res_got)

    back, total, held = lax.optimization_barrier((backs[0], total, held))
    back_got = keep_in_vmem(lax.ppermute(back, "seq", swap_core))
    held = pl.pallas_call(
        functools.partial(overlay_kernel, rows, heads),
        in_specs=[smem] + [vmem] * 5,
        out_specs=[vmem] * 4,
        out_shape=[pltpu.VMEM((rows, width), bf16)] * 4,
        input_output_aliases={2 + i: i for i in range(4)},
        scratch_shapes=[pltpu.VMEM((4, length + 2 * rows, D_HEAD), bf16)],
        compiler_params=limit(4),
        name="overlay",
    )(plan, keep_in_vmem(back), *[keep_in_vmem(x) for x in held])

    full = jax.ShapeDtypeStruct((rows, width), bf16)
    args = [plan, raw_q, raw_k, q_gain2, k_gain2, keep_in_vmem(inv)]
    args += [keep_in_vmem(total), keep_in_vmem(total_got), back_got]
    args += [keep_in_vmem(x) for x in held]
    outs = pl.pallas_call(
        functools.partial(finish_kernel, rows, heads),
        in_specs=[smem] + [vmem] * (len(args) - 1),
        out_specs=[hbm] * 6 + [vmem] * 4,
        out_shape=[full] * 4
        + [jax.ShapeDtypeStruct((CORES * heads, D_HEAD), f32)] * 2
        + [pltpu.VMEM((rows, width), bf16)] * 4,
        input_output_aliases={len(args) - 4 + i: 6 + i for i in range(4)},
        scratch_shapes=[
            pltpu.VMEM((4, length + 2 * rows, D_HEAD), bf16),
            pltpu.VMEM((rows, width), bf16),
            pltpu.VMEM((rows, width), bf16),
            pltpu.VMEM((2, CORES * heads, D_HEAD), f32),
            pltpu.SemaphoreType.DMA((8,)),
        ],
        compiler_params=pltpu.CompilerParams(vmem_limit_bytes=12 << 20),
        name="finish",
    )(*args)
    attn_out, query_grad, key_grad, value_grad = outs[:4]
    return (attn_out, query_grad, key_grad, value_grad, *(x.reshape(width) for x in outs[4:6]))


def solution(mesh):
    dp, seq = mesh.shape["dp"], mesh.shape["seq"]
    two_chips = seq == 2 * CORES and dp > 1 and dp & (dp - 1) == 0

    def per_device(queries, keys, values, q_gain, k_gain, out_grad, segments, visible):
        args = (queries, keys, values, q_gain, k_gain, out_grad, segments, visible)
        if two_chips:
            return per_device_clips(*args, dp)
        return per_device_any(*args)

    rows = P(("dp", "seq"), None)
    return jax.shard_map(
        per_device,
        mesh=mesh,
        in_specs=(rows, rows, rows, P(), P(), rows, P("dp", None), P("dp", None)),
        out_specs=(rows, rows, rows, rows, P(), P()),
        check_vma=False,
    )
```
